32 devices in a mesh: dom: 8 (over z, x), dir: 4 (over y, core).
Axes of the slice: x: 2, y: 2, z: 4, core: 2. Of those that a mesh axis runs over, the one named last changes fastest.
Arguments:
- x_edges: bfloat16 [65536, 128], P(('dom', 'dir')), may hold values from -6 to 6
- send_list: int32 [1024, 32], P(('dom', 'dir')), may hold values from 0 to 2048, as said below
- connectivity: int32 [6, 32768], P(None, ('dom', 'dir')), may hold values from 0 to 3071, as said below
- elem_mats: float32 [36, 32768], P(None, ('dom', 'dir'))
- elem_live: int32 [32], P(('dom', 'dir')), may hold values from 512 to 1024, as said below
- currents: bfloat16 [1024, 128, 128], P(('dom', 'dir')), may hold values from -0.1796875 to 0.1796875
- positions: bfloat16 [1024, 3, 128], P(('dom', 'dir')), may hold values from -1 to 1
- block_live: int32 [1024], P(('dom', 'dir')), may hold values from 32 to 128
- block_owner: int32 [1024], P(('dom', 'dir')), may hold values from 0 to 7, as said below
- block_leaf: int32 [1024], P(('dom', 'dir')), may hold values from 0 to 15
- cone_waves: float32 [3, 16], P(None, 'dir'), may hold values from -6 to 6
Outputs:
- interior_out: float32 [65536, 128], P(('dom', 'dir'))
- expansions: float32 [16, 16, 2, 64, 128], P('dom', 'dir')
The draws below stay inside these ranges and needn't reach their ends.
Inputs may be any that keep to these rules, and one draw needn't show every extreme that they name: `send_list`: in row a * 32 + b the used entries come first and name owned edges of a; the rest are 2048. A partition reads nothing of itself; some pair uses all 32 entries. `connectivity`: entries below 2048 are owned edges; 2048 + p * 32 + s names the s-th edge that partition p lists for this partition, and only used entries are named. `elem_live`: elements at positions from this count on are padding; some partition has all 1024. `block_owner`: among the 32 blocks of one partition at most 12 name one leaf owner; some leaf owner is named by exactly 12 blocks of every partition.
All inputs are finite; a program needn't handle non-finite values.
Results may differ from the reference program's by a relative error of at most 0.0056.
Values may be sent and summed in bfloat16 or wider, within the bound.
A program may use at most 128 MiB of HBM per device.

```python
import jax
import jax.numpy as jnp
from jax import lax

E_OWN = 2048
EL_DEV = 1024
HS = 32
NRHS = 128
BS = 128
BLK_DEV = 32
LEAVES_DEV = 16
NODES = 4
PARTITIONS = 32
OWNERS = 8
EDGES = 65536
ELEMENTS = 32768
BLOCKS = 1024
CAP = 12
LEAVES = 128
CONES = 16


def halo_counts(key):
    base_key = jax.random.fold_in(key, 7001)
    first_key, second_key, third_key, extra_key = jax.random.split(base_key, 4)
    counts = jax.random.randint(first_key, (PARTITIONS, PARTITIONS), HS // 2, HS + 1)
    rows_now = jnp.arange(PARTITIONS)[:, None]
    cols_now = jnp.arange(PARTITIONS)[None, :]
    distance = (cols_now - rows_now) % PARTITIONS
    nearby = (distance >= 1) & (distance <= 8) | (distance >= PARTITIONS - 8)
    further = jax.random.randint(extra_key, (PARTITIONS, PARTITIONS), 0, PARTITIONS) < 4
    linked = (nearby | further) & (distance != 0)
    counts = jnp.where(linked, counts, 0)
    sender = jax.random.randint(second_key, (), 0, PARTITIONS)
    stride = jax.random.randint(third_key, (), 1, PARTITIONS)
    return counts.at[sender, (sender + stride) % PARTITIONS].set(HS)


def draw_send_list(key, part):
    counts = halo_counts(key)
    entries = jax.random.randint(jax.random.fold_in(key, 7002), (PARTITIONS * PARTITIONS, HS), 0, E_OWN)
    used_slots = jnp.arange(HS)[None, :] < counts.reshape(-1)[:, None]
    return jnp.where(used_slots, entries, E_OWN).astype(jnp.int32)


def draw_connectivity(key, part):
    counts = halo_counts(key)
    incoming = counts.T
    running = jnp.cumsum(incoming, axis=1)
    totals = running[:, -1]
    keys_all = jax.random.split(jax.random.fold_in(key, 7003), 3)
    width_all = 6 * EL_DEV
    picks = jax.random.randint(keys_all[0], (PARTITIONS, width_all), 0, 1048576) % jnp.maximum(totals, 1)[:, None]
    sender = jax.vmap(lambda row_sums, wanted: jnp.searchsorted(row_sums, wanted, side='right'))(running, picks)
    sender = jnp.minimum(sender.astype(jnp.int32), PARTITIONS - 1)
    before = jnp.take_along_axis(running, sender, axis=1) - jnp.take_along_axis(incoming, sender, axis=1)
    halo_index = E_OWN + sender * HS + (picks - before)
    local_index = jax.random.randint(keys_all[1], (PARTITIONS, width_all), 0, E_OWN)
    choose_halo = (jax.random.randint(keys_all[2], (PARTITIONS, width_all), 0, 4) == 0) & (totals[:, None] > 0)
    merged = jnp.where(choose_halo, halo_index, local_index)
    return merged.reshape(PARTITIONS, 6, EL_DEV).transpose(1, 0, 2).reshape(6, PARTITIONS * EL_DEV).astype(jnp.int32)


def draw_elem_mats(key, part):
    first_key, second_key = jax.random.split(jax.random.fold_in(key, 7004), 2)
    random_part = jax.random.uniform(first_key, (6, 6, ELEMENTS), jnp.float32, -0.35, 0.35)
    symmetric = 0.5 * (random_part + random_part.transpose(1, 0, 2))
    identity = jnp.eye(6, dtype=jnp.float32)[:, :, None]
    offdiag = symmetric * (1.0 - identity)
    lifted = jnp.sum(jnp.abs(offdiag), axis=1) + jax.random.uniform(second_key, (6, ELEMENTS), jnp.float32, 0.5, 1.5)
    matrix = offdiag + identity * lifted[:, None, :]
    return (0.3 * matrix).reshape(36, ELEMENTS)


def draw_elem_live(key, part):
    first_key, second_key = jax.random.split(jax.random.fold_in(key, 7005))
    counts = jax.random.randint(first_key, (PARTITIONS,), EL_DEV // 2, EL_DEV + 1)
    fullest = jax.random.randint(second_key, (), 0, PARTITIONS)
    return counts.at[fullest].set(EL_DEV).astype(jnp.int32)


def draw_block_owner(key, part):
    base_key = jax.random.fold_in(key, 7006)
    hot_key, device_key = jax.random.split(base_key)
    hottest = jax.random.randint(hot_key, (), 0, OWNERS)
    others = BLK_DEV - CAP

    def one_device(device):
        spread_key, order_key = jax.random.split(jax.random.fold_in(device_key, device))
        places = jax.random.permutation(spread_key, (OWNERS - 1) * CAP)[:others] // CAP
        places = jnp.where(places >= hottest, places + 1, places)
        owners_now = jnp.concatenate([jnp.full((CAP,), hottest, jnp.int32), places.astype(jnp.int32)])
        return owners_now[jax.random.permutation(order_key, BLK_DEV)]
    return jax.vmap(one_device)(jnp.arange(PARTITIONS)).reshape(-1).astype(jnp.int32)


def draw_positions(key, part):
    first_key = jax.random.fold_in(jax.random.fold_in(key, 7007), 0)
    values = jax.random.uniform(first_key, (BLOCKS, 3, BS), jnp.float32, -1.0, 1.0)
    return values.astype(jnp.bfloat16)


def draw_cone_waves(key, part):
    first_key, second_key = jax.random.split(jax.random.fold_in(key, 7008))
    magnitude = jax.random.uniform(first_key, (3, CONES), jnp.float32, 5.0, 6.0)
    signs = jnp.where(jax.random.uniform(second_key, (3, CONES), jnp.float32) < 0.5, -1.0, 1.0)
    return (signs * magnitude).astype(jnp.float32)


def touch_ends(values, key, smallest, top_value):
    longest = values.shape.index(max(values.shape))
    spots = []
    for shift in (0, 1):
        where = [jax.random.randint(jax.random.fold_in(key, axis), (), 0, length) for axis, length in enumerate(values.shape)]
        where[longest] = (where[longest] + shift) % values.shape[longest]
        spots.append(tuple(where))
    return values.at[spots[0]].set(smallest).at[spots[1]].set(top_value)


def steps_of(rng, extent, cuts, smallest, high):
    def one(position, blocks):
        steps = jax.random.uniform(jax.random.fold_in(jax.random.fold_in(rng, 6), position), (blocks,), jnp.float32, smallest / len(cuts), high / len(cuts))
        return jnp.repeat(jnp.exp(steps), extent[position] // blocks).reshape((-1,) + (1,) * (len(extent) - position - 1))

    level = one(*cuts[0])
    for cut in cuts[1:]:
        level = level * one(*cut)
    return level


def gaussian(stream_key, shape, width, bound, shards=(), held_as=jnp.bfloat16):
    level = steps_of(stream_key, shape, shards, -0.22, 0.18) if shards else 1.0
    array = jax.random.normal(stream_key, shape, jnp.float32) * width * level
    return jnp.minimum(jnp.maximum(array, -bound), bound).astype(held_as)


def setup_inputs(seed: int = 0) -> dict:
    seeds = jax.random.split(jax.random.key(seed), 12)
    x_edges = gaussian(seeds[0], (EDGES, NRHS), 1.0, 6.0, ((0, 32),))
    send_list = draw_send_list(jax.random.fold_in(seeds[11], 71), 0)
    connectivity = draw_connectivity(jax.random.fold_in(seeds[11], 71), 0)
    elem_mats = draw_elem_mats(jax.random.fold_in(seeds[11], 71), 0)
    elem_live = draw_elem_live(jax.random.fold_in(seeds[11], 71), 0)
    currents = gaussian(seeds[5], (BLOCKS, BS, NRHS), 0.03, 0.1796875, ((0, 32),))
    positions = draw_positions(jax.random.fold_in(seeds[11], 71), 0)
    block_live = touch_ends(jax.random.randint(seeds[7], (BLOCKS,), BS // 4, BS + 1), jax.random.fold_in(seeds[7], 1), BS // 4, BS).astype(jnp.int32)
    block_owner = draw_block_owner(jax.random.fold_in(seeds[11], 71), 0)
    block_leaf = touch_ends(jax.random.randint(seeds[9], (BLOCKS,), 0, LEAVES_DEV), jax.random.fold_in(seeds[9], 1), 0, LEAVES_DEV - 1).astype(jnp.int32)
    cone_waves = draw_cone_waves(jax.random.fold_in(seeds[11], 71), 0)
    return {"x_edges": x_edges, "send_list": send_list, "connectivity": connectivity, "elem_mats": elem_mats, "elem_live": elem_live, "currents": currents, "positions": positions, "block_live": block_live, "block_owner": block_owner, "block_leaf": block_leaf, "cone_waves": cone_waves}


def cheb_points():
    node_order = jnp.arange(NODES).astype(jnp.float32)
    return jnp.cos((2.0 * node_order + 1.0) * (jnp.pi / (2.0 * NODES)))


def lagrange(points):
    node_values = cheb_points()
    rows_out = []
    for target in range(NODES):
        product = jnp.ones_like(points)
        for other_node in range(NODES):
            if other_node != target:
                product = product * (points - node_values[other_node]) / (node_values[target] - node_values[other_node])
        rows_out.append(product)
    return jnp.stack(rows_out, axis=-2)


def tensor_basis(coords):
    first = lagrange(coords[..., 0, :])
    second = lagrange(coords[..., 1, :])
    third = lagrange(coords[..., 2, :])
    joined = first[..., :, None, None, :] * second[..., None, :, None, :] * third[..., None, None, :, :]
    return joined.reshape(coords.shape[:-2] + (NODES ** 3, coords.shape[-1]))


def node_coords():
    ladder = jnp.arange(NODES ** 3)
    digits = jnp.stack([ladder // (NODES * NODES), (ladder // NODES) % NODES, ladder % NODES]).astype(jnp.float32)
    return jnp.cos((2.0 * digits + 1.0) * (jnp.pi / (2.0 * NODES)))


def wave_phase(waves, coords):
    return (waves[0][:, None] * coords[..., None, 0, :] + waves[1][:, None] * coords[..., None, 1, :]
            + waves[2][:, None] * coords[..., None, 2, :])


def m2m_tables(waves):
    octant = jnp.arange(8)
    shifts = jnp.stack([octant // 4, (octant // 2) % 2, octant % 2], axis=1).astype(jnp.float32) - 0.5
    points = shifts[:, :, None] + 0.5 * cheb_points()[None, None, :]
    weights = lagrange(points)
    first = weights[:, 0]
    second = weights[:, 1]
    third = weights[:, 2]
    joined = first[:, :, None, None, :, None, None] * second[:, None, :, None, None, :, None] * third[:, None, None, :, None, None, :]
    square = NODES ** 3
    joined = joined.reshape(8, square, square)
    child = shifts[:, :, None] + 0.5 * node_coords()[None]
    spread = child[:, :, None, :] - node_coords()[None, :, :, None]
    psi = 2.0 * (waves[0][:, None, None, None] * spread[None, :, 0] + waves[1][:, None, None, None] * spread[None, :, 1]
                 + waves[2][:, None, None, None] * spread[None, :, 2])
    table_real = (joined[None] * jnp.cos(psi)).astype(jnp.bfloat16)
    table_imag = (-joined[None] * jnp.sin(psi)).astype(jnp.bfloat16)
    return table_real, table_imag


def interior_product(x_edges, send_list, connectivity, elem_mats, elem_live):
    total_rows = x_edges.shape[0]
    columns = x_edges.shape[1]

    def one_part(accumulated, device):
        local_links = lax.dynamic_slice_in_dim(connectivity, device * EL_DEV, EL_DEV, 1)
        matrices = lax.dynamic_slice_in_dim(elem_mats, device * EL_DEV, EL_DEV, 1)
        offset = jnp.maximum(local_links - E_OWN, 0)
        sender = offset // HS
        listed = send_list[sender * PARTITIONS + device, offset % HS]
        global_rows = jnp.where(local_links < E_OWN, device * E_OWN + local_links, sender * E_OWN + listed).astype(jnp.int32)
        gathered = x_edges[global_rows]
        live_mask = (jnp.arange(EL_DEV) < elem_live[device])[:, None]
        term_list = []
        for row_index in range(6):
            summed = jnp.zeros((EL_DEV, columns), jnp.float32)
            for col_index in range(6):
                summed = summed + matrices[row_index * 6 + col_index][:, None] * gathered[col_index].astype(jnp.float32)
            term_list.append(jnp.where(live_mask, summed, jnp.zeros_like(summed)))
        stacked = jnp.stack(term_list).reshape(6 * EL_DEV, columns)
        return accumulated.at[global_rows.reshape(-1)].add(stacked), None

    initial = jnp.zeros((total_rows, columns), jnp.float32)
    result, unused = lax.scan(one_part, initial, jnp.arange(PARTITIONS, dtype=jnp.int32))
    return result


def boundary_product(currents, positions, block_live, block_owner, block_leaf, cone_waves):
    cone_total = cone_waves.shape[1]
    columns = currents.shape[2]
    square = NODES ** 3
    live_mask = jnp.arange(BS)[None, :] < block_live[:, None]
    masked = jnp.where(live_mask[:, :, None], currents, jnp.zeros_like(currents))
    leaf_index = (block_owner * LEAVES_DEV + block_leaf).astype(jnp.int32)
    batches = BLOCKS // 128

    def one_batch(carry, inputs):
        real_sum, imag_sum = carry
        blocks_now, coords, leaves = inputs
        coords_wide = coords.astype(jnp.float32)
        basis_now = tensor_basis(coords_wide)
        phase_now = wave_phase(cone_waves, coords_wide)
        real_w = (basis_now[:, None] * jnp.cos(phase_now)[:, :, None, :]).astype(jnp.bfloat16)
        imag_w = (-basis_now[:, None] * jnp.sin(phase_now)[:, :, None, :]).astype(jnp.bfloat16)
        block_data = blocks_now.astype(jnp.float32)
        real_part = jnp.einsum("gcqb,gbn->gcqn", real_w.astype(jnp.float32), block_data).astype(jnp.bfloat16)
        imag_part = jnp.einsum("gcqb,gbn->gcqn", imag_w.astype(jnp.float32), block_data).astype(jnp.bfloat16)
        real_sum = real_sum.at[leaves].add(real_part.astype(jnp.float32))
        imag_sum = imag_sum.at[leaves].add(imag_part.astype(jnp.float32))
        return (real_sum, imag_sum), None

    empty = jnp.zeros((LEAVES, cone_total, square, columns), jnp.float32)
    inputs = (masked.reshape(batches, 128, BS, columns), positions.reshape(batches, 128, 3, BS), leaf_index.reshape(batches, 128))
    sums, unused = lax.scan(one_batch, (empty, empty), inputs)
    real_sum, imag_sum = sums
    node_phase = wave_phase(cone_waves, node_coords())
    cosine = jnp.cos(node_phase)[None, :, :, None]
    sine_part = jnp.sin(node_phase)[None, :, :, None]
    leaf_real = (cosine * real_sum - sine_part * imag_sum).astype(jnp.bfloat16)
    leaf_imag = (cosine * imag_sum + sine_part * real_sum).astype(jnp.bfloat16)
    table_real, table_imag = m2m_tables(cone_waves)
    child_real = leaf_real.reshape(LEAVES // 8, 8, cone_total, square, columns).astype(jnp.float32)
    child_imag = leaf_imag.reshape(LEAVES // 8, 8, cone_total, square, columns).astype(jnp.float32)
    wide_real = table_real.astype(jnp.float32)
    wide_imag = table_imag.astype(jnp.float32)
    parent_real = jnp.einsum("cops,xocsn->xcpn", wide_real, child_real) - jnp.einsum("cops,xocsn->xcpn", wide_imag, child_imag)
    parent_imag = jnp.einsum("cops,xocsn->xcpn", wide_real, child_imag) + jnp.einsum("cops,xocsn->xcpn", wide_imag, child_real)
    return jnp.stack([parent_real, parent_imag], axis=2)


def reference(x_edges, send_list, connectivity, elem_mats, elem_live, currents, positions, block_live, block_owner, block_leaf, cone_waves):
    interior_out = interior_product(x_edges, send_list, connectivity, elem_mats, elem_live)
    expansions = boundary_product(currents, positions, block_live, block_owner, block_leaf, cone_waves)
    return (interior_out, expansions)
```

```python
import math

import jax
import jax.numpy as jnp
from jax import lax
from jax.experimental import pallas as pl
from jax.experimental.pallas import tpu as pltpu
from jax.sharding import PartitionSpec as P

LEAVES_DEV = 16
OCTANTS = 8
NODES = 4
PLANE = NODES * NODES
SQUARE = NODES**3
POINTS = [math.cos((2 * j + 1) * math.pi / (2 * NODES)) for j in range(NODES)]
META = 6


def lagrange_rows(v):
    rows = []
    for target in range(NODES):
        product = None
        scale = 1.0
        for other in range(NODES):
            if other != target:
                factor = v - POINTS[other]
                product = factor if product is None else product * factor
                scale *= POINTS[target] - POINTS[other]
        rows.append(product * (1.0 / scale))
    return rows


def cos_sin(phase):
    turns = jnp.floor(phase * (1.0 / math.pi) + 0.5)
    odd = turns - 2.0 * jnp.floor(turns * 0.5)
    sign = 1.0 - 2.0 * odd
    high = 3.140625
    rest = (phase - turns * high) - turns * (math.pi - high)
    square = rest * rest
    cosine = jnp.full_like(rest, 1.0 / math.factorial(12))
    for order in (10, 8, 6, 4, 2, 0):
        cosine = cosine * square + (1.0 if order % 4 == 0 else -1.0) / math.factorial(order)
    sine = jnp.full_like(rest, -1.0 / math.factorial(11))
    for order in (9, 7, 5, 3, 1):
        sine = sine * square + (1.0 if order % 4 == 1 else -1.0) / math.factorial(order)
    return cosine * sign, sine * rest * sign


def xor_pairs(count, bit):
    return [(i, i ^ (1 << bit)) for i in range(count)]


def log2(count):
    bits = count.bit_length() - 1
    if count != 1 << bits:
        raise ValueError("axis size")
    return bits


def spread(value, axis, bits):
    held = [value]
    count = lax.axis_size(axis)
    for bit in bits:
        held = held + [lax.ppermute(h, axis, xor_pairs(count, bit)) for h in held]
    return held


def block_sums(slots, waves, metas, blocks, previous, slot_count, cone_count, chunks):
    lists = len(metas)
    per_list, block_size, columns = blocks[0].shape
    height = 2 * cone_count * SQUARE
    firsts = 2 * cone_count * NODES
    rows = PLANE + firsts
    group = 16
    half = slot_count // 2
    piece = height // chunks if chunks else height

    def kernel(*refs):
        slot_ref, wave_ref = refs[:2]
        meta_refs = refs[2 : 2 + lists]
        block_refs = refs[2 + lists : 2 + 2 * lists]
        at = 2 + 2 * lists
        if previous is not None:
            before_ref = refs[at]
            at += 1
        outs = refs[at:-2] if chunks else refs[at:-1]
        factor_ref = refs[-1]
        sum_ref = refs[-2] if chunks else outs[0]

        for which in range(lists):
            for part in range(per_list // group):
                span = pl.ds(part * group, group)
                meta = [meta_refs[which][row, span, :].astype(jnp.float32) for row in range(META)]
                octant = meta[3] - 8.0 * jnp.floor(meta[3] * 0.125)
                high = jnp.floor(octant * 0.25)
                middle = jnp.floor((octant - 4.0 * high) * 0.5)
                low = octant - 4.0 * high - 2.0 * middle
                double = [2.0 * bit - 1.0 + pos for bit, pos in zip((high, middle, low), meta[:3])]
                lanes = lax.broadcasted_iota(jnp.int32, (group, block_size), 1).astype(jnp.float32)
                live = lanes < meta[4]
                first = [jnp.where(live, r, 0.0) for r in lagrange_rows(0.5 * double[0])]
                second = lagrange_rows(0.5 * double[1])
                third = lagrange_rows(0.5 * double[2])
                start = (which * per_list + part * group) * rows

                def put(row, value):
                    factor_ref[pl.ds(start + row, group, stride=rows), :] = value

                for a in range(NODES):
                    for b in range(NODES):
                        put(a * NODES + b, second[a] * third[b])
                for cone in range(cone_count):
                    phase = (
                        wave_ref[0, cone] * double[0]
                        + wave_ref[1, cone] * double[1]
                        + wave_ref[2, cone] * double[2]
                    )
                    cosine, sine = cos_sin(phase)
                    for digit in range(NODES):
                        put(PLANE + cone * 2 * NODES + digit, first[digit] * cosine)
                        put(PLANE + cone * 2 * NODES + NODES + digit, first[digit] * -sine)

        sum_ref[...] = jnp.zeros_like(sum_ref)
        for which in range(lists):

            def one(index, carry):
                base = pl.multiple_of((which * per_list + index) * rows, 8)
                pairs = factor_ref[pl.ds(base, PLANE), :]
                pieces = [
                    (factor_ref[pl.ds(base + PLANE + row, 1), :] * pairs).astype(jnp.bfloat16)
                    for row in range(firsts)
                ]
                weights = jnp.concatenate(pieces, axis=0)
                product = jnp.dot(
                    weights, block_refs[which][index], preferred_element_type=jnp.float32
                )
                slot = slot_ref[which * per_list + index]
                sum_ref[slot] += product
                return carry

            lax.fori_loop(0, per_list, one, 0, unroll=2)

        if chunks:

            def finish(slot, carry):
                for chunk in range(chunks):
                    span = pl.ds(chunk * piece, piece)
                    keep = sum_ref[slot, span, :]
                    send = sum_ref[half + slot, span, :]
                    if previous is not None:
                        keep += before_ref[slot, span, :]
                        send += before_ref[half + slot, span, :]
                    outs[chunk][slot] = keep
                    outs[chunks + chunk][slot] = send.astype(jnp.bfloat16)
                return carry

            lax.fori_loop(0, half, finish, 0)

    whole = jax.ShapeDtypeStruct((slot_count, height, columns), jnp.float32)
    if chunks:
        out_shape = [jax.ShapeDtypeStruct((half, piece, columns), jnp.float32)] * chunks + [
            jax.ShapeDtypeStruct((half, piece, columns), jnp.bfloat16)
        ] * chunks
    else:
        out_shape = [whole]
    vmem = pl.BlockSpec(memory_space=pltpu.VMEM)
    smem = pl.BlockSpec(memory_space=pltpu.SMEM)
    scratch = [pltpu.VMEM((lists * per_list * rows, block_size), jnp.float32)]
    if chunks:
        scratch = [pltpu.VMEM(whole.shape, jnp.float32)] + scratch
    operands = [slots, waves, *metas, *blocks] + ([previous] if previous is not None else [])
    total = lists * per_list
    return pl.pallas_call(
        kernel,
        out_shape=out_shape,
        in_specs=[smem, smem] + [vmem] * (len(operands) - 2),
        out_specs=[vmem] * len(out_shape),
        scratch_shapes=scratch,
        compiler_params=pltpu.CompilerParams(vmem_limit_bytes=48 << 20),
        cost_estimate=pl.CostEstimate(
            flops=2 * total * height * block_size * columns,
            bytes_accessed=total * block_size * columns * 2 + slot_count * height * columns * 4,
            transcendentals=0,
        ),
    )(*operands)


def boundary_part(currents, positions, block_live, block_owner, block_leaf, cone_waves):
    block_count, block_size, columns = currents.shape
    cone_count = cone_waves.shape[1]
    dom_count, dir_count = lax.axis_size("dom"), lax.axis_size("dir")
    parents = LEAVES_DEV // OCTANTS
    slot_count = dom_count * parents
    dom_bits, dir_bits = log2(dom_count), log2(dir_count)

    numbers = jnp.stack([block_leaf, block_live, block_owner]).astype(jnp.bfloat16)
    meta = jnp.concatenate(
        [
            positions.transpose(1, 0, 2),
            jnp.broadcast_to(numbers[:, :, None], (3, block_count, block_size)),
        ],
        axis=0,
    )
    low = list(range(dir_bits - 1))
    groups = []
    far = lax.ppermute(currents, "dir", xor_pairs(dir_count, dir_bits - 1))
    far_meta = lax.ppermute(meta, "dir", xor_pairs(dir_count, dir_bits - 1))
    groups.append((spread(meta, "dir", low), spread(currents, "dir", low)))
    groups.append((spread(far_meta, "dir", low), spread(far, "dir", low)))

    me = lax.axis_index("dom")

    def slots_of(metas):
        ints = jnp.stack([m[3:META, :, 0] for m in metas], axis=1).astype(jnp.int32)
        leaf, owner = ints[0].reshape(-1), ints[2].reshape(-1)
        relative = owner ^ me
        order = jnp.zeros_like(relative)
        for bit in range(dom_bits):
            order = order | (((relative >> bit) & 1) << (dom_bits - 1 - bit))
        return order * parents + leaf // OCTANTS

    chunks = cone_count
    (near,) = block_sums(
        slots_of(groups[0][0]), cone_waves, *groups[0], None, slot_count, cone_count, 0
    )
    pieces = block_sums(
        slots_of(groups[1][0]), cone_waves, *groups[1], near, slot_count, cone_count, chunks
    )
    keeps, sends = list(pieces[:chunks]), list(pieces[chunks:])
    size = slot_count // 2
    for bit in range(dom_bits):
        next_keeps, next_sends = [], []
        for keep, send in zip(keeps, sends):
            got = lax.ppermute(send, "dom", xor_pairs(dom_count, bit))
            if bit < dom_bits - 1:
                lower = size // 2
                next_keeps.append(keep[:lower] + got[:lower].astype(jnp.float32))
                next_sends.append(
                    (keep[lower:] + got[lower:].astype(jnp.float32)).astype(jnp.bfloat16)
                )
            else:
                next_keeps.append(keep + got.astype(jnp.float32))
        keeps, sends = next_keeps, next_sends
        size //= 2
    digits = jnp.arange(SQUARE)
    digits = jnp.stack([digits // PLANE, digits // NODES % NODES, digits % NODES])
    nodes = jnp.cos((2.0 * digits.astype(jnp.float32) + 1.0) * (math.pi / (2.0 * NODES)))
    angle = 2.0 * (
        cone_waves[0][:, None] * nodes[0]
        + cone_waves[1][:, None] * nodes[1]
        + cone_waves[2][:, None] * nodes[2]
    )
    cosine, sine = jnp.cos(angle), jnp.sin(angle)
    outs = []
    per = cone_count // chunks
    for chunk, keep in enumerate(keeps):
        parts = keep.reshape(parents, per, 2, SQUARE, columns)
        c = cosine[chunk * per : (chunk + 1) * per][None, :, :, None]
        s = sine[chunk * per : (chunk + 1) * per][None, :, :, None]
        real, imag = parts[:, :, 0], parts[:, :, 1]
        outs.append(jnp.stack([c * real - s * imag, c * imag + s * real], axis=2))
    return jnp.concatenate(outs, axis=1)


def element_sums(links, live, x_edges, received, mats, owned_rows):
    edges, element_count = links.shape
    columns = x_edges.shape[1]
    halo = received.shape[0]
    table_rows = owned_rows + halo
    step = 8

    def kernel(link_ref, live_ref, x_ref, halo_ref, mat_ref, own_ref, back_ref, *scratch):
        table_ref, got_ref, term_ref = scratch[:3]
        sums = scratch[3:]
        table_ref[pl.ds(0, owned_rows), :] = x_ref[...].astype(jnp.float32)
        table_ref[pl.ds(owned_rows, halo), :] = halo_ref[...].astype(jnp.float32)
        for ref in sums:
            ref[...] = jnp.zeros_like(ref)

        def one(index, carry):
            start = pl.multiple_of(index * step, step)
            for edge in range(edges):
                for lane in range(step):
                    row = link_ref[edge, start + lane]
                    got_ref[edge, pl.ds(lane, 1), :] = table_ref[pl.ds(row, 1), :]
            number = start + lax.broadcasted_iota(jnp.int32, (step, mat_ref.shape[1]), 0)
            mat = jnp.where(number < live_ref[0], mat_ref[pl.ds(start, step), :], 0.0)
            got = [got_ref[edge] for edge in range(edges)]
            for i in range(edges):
                total = None
                for j in range(edges):
                    at = edges * i + j
                    term = mat[:, at : at + 1] * got[j]
                    total = term if total is None else total + term
                term_ref[i] = total
            for lane in range(step):
                for edge in range(edges):
                    row = link_ref[edge, start + lane]
                    sums[edge][pl.ds(row, 1), :] += term_ref[edge, pl.ds(lane, 1), :]
            return carry

        lax.fori_loop(0, element_count // step, one, 0)

        def total_of(span):
            total = sums[0][span, :]
            for ref in sums[1:]:
                total = total + ref[span, :]
            return total

        own_ref[...] = total_of(pl.ds(0, owned_rows))
        back_ref[...] = total_of(pl.ds(owned_rows, halo)).astype(jnp.bfloat16)

    vmem = pl.BlockSpec(memory_space=pltpu.VMEM)
    smem = pl.BlockSpec(memory_space=pltpu.SMEM)
    return pl.pallas_call(
        kernel,
        out_shape=[
            jax.ShapeDtypeStruct((owned_rows, columns), jnp.float32),
            jax.ShapeDtypeStruct((halo, columns), jnp.bfloat16),
        ],
        in_specs=[smem, smem, vmem, vmem, vmem],
        out_specs=[vmem, vmem],
        scratch_shapes=[
            pltpu.VMEM((table_rows, columns), jnp.float32),
            pltpu.VMEM((edges, step, columns), jnp.float32),
            pltpu.VMEM((edges, step, columns), jnp.float32),
        ]
        + [pltpu.VMEM((table_rows, columns), jnp.float32)] * edges,
        compiler_params=pltpu.CompilerParams(vmem_limit_bytes=56 << 20),
        cost_estimate=pl.CostEstimate(
            flops=4_000_000_000, bytes_accessed=table_rows * columns * 8, transcendentals=0
        ),
    )(links, live, x_edges, received, mats)


def fold_sums(rows, returned, owned):
    count, columns = returned.shape
    owned_rows = owned.shape[0]
    ways = 4

    def kernel(row_ref, back_ref, own_ref, out_ref, wide_ref, *sums):
        wide_ref[...] = back_ref[...].astype(jnp.float32)
        for ref in sums:
            ref[...] = jnp.zeros_like(ref)

        def one(index, carry):
            start = pl.multiple_of(index * 16, 16)
            for lane in range(16):
                row = row_ref[start + lane]
                sums[lane % ways][pl.ds(row, 1), :] += wide_ref[pl.ds(start + lane, 1), :]
            return carry

        lax.fori_loop(0, count // 16, one, 0)
        total = own_ref[...]
        for ref in sums:
            total = total + ref[...]
        out_ref[...] = total

    vmem = pl.BlockSpec(memory_space=pltpu.VMEM)
    return pl.pallas_call(
        kernel,
        out_shape=jax.ShapeDtypeStruct((owned_rows, columns), jnp.float32),
        in_specs=[pl.BlockSpec(memory_space=pltpu.SMEM), vmem, vmem],
        out_specs=vmem,
        scratch_shapes=[pltpu.VMEM((count, columns), jnp.float32)]
        + [pltpu.VMEM((owned_rows, columns), jnp.float32)] * ways,
        cost_estimate=pl.CostEstimate(
            flops=1_000_000_000, bytes_accessed=owned_rows * columns * 8, transcendentals=0
        ),
    )(rows, returned, owned)


def interior_part(x_edges, send_list, connectivity, elem_mats, elem_live):
    owned_rows, columns = x_edges.shape
    partitions, slot_width = send_list.shape
    rows = jnp.minimum(send_list, owned_rows - 1)
    outgoing = x_edges[rows]
    received = lax.all_to_all(outgoing, ("dom", "dir"), split_axis=0, concat_axis=0, tiled=True)
    owned, back = element_sums(
        connectivity,
        elem_live,
        x_edges,
        received.reshape(partitions * slot_width, columns),
        elem_mats.T,
        owned_rows,
    )
    returned = lax.all_to_all(
        back.reshape(partitions, slot_width, columns),
        ("dom", "dir"),
        split_axis=0,
        concat_axis=0,
        tiled=True,
    )
    return fold_sums(rows.reshape(-1), returned.reshape(partitions * slot_width, columns), owned)


def shards(
    x_edges,
    send_list,
    connectivity,
    elem_mats,
    elem_live,
    currents,
    positions,
    block_live,
    block_owner,
    block_leaf,
    cone_waves,
):
    interior_out = interior_part(x_edges, send_list, connectivity, elem_mats, elem_live)
    expansions = boundary_part(currents, positions, block_live, block_owner, block_leaf, cone_waves)
    return (interior_out, expansions)


def solution(mesh):
    placed = (
        P(("dom", "dir"), None),
        P(("dom", "dir"), None),
        P(None, ("dom", "dir")),
        P(None, ("dom", "dir")),
        P(("dom", "dir")),
        P(("dom", "dir"), None, None),
        P(("dom", "dir"), None, None),
        P(("dom", "dir")),
        P(("dom", "dir")),
        P(("dom", "dir")),
        P(None, "dir"),
    )
    return jax.shard_map(
        shards,
        mesh=mesh,
        in_specs=placed,
        out_specs=(P(("dom", "dir"), None), P("dom", "dir", None, None, None)),
        check_vma=False,
    )
```

```python
import math

import jax
import jax.numpy as jnp
from jax import lax
from jax.experimental import pallas as pl
from jax.experimental.pallas import tpu as pltpu
from jax.sharding import PartitionSpec as P

LEAVES_DEV = 16
OCTANTS = 8
NODES = 4
PLANE = NODES * NODES
SQUARE = NODES**3
POINTS = [math.cos((2 * j + 1) * math.pi / (2 * NODES)) for j in range(NODES)]
MESH = pl.DeviceIdType.MESH
VMEM = pl.BlockSpec(memory_space=pltpu.VMEM)
SMEM = pl.BlockSpec(memory_space=pltpu.SMEM)


def lagrange_rows(v):
    rows = []
    for target in range(NODES):
        product = None
        scale = 1.0
        for other in range(NODES):
            if other != target:
                factor = v - POINTS[other]
                product = factor if product is None else product * factor
                scale *= POINTS[target] - POINTS[other]
        rows.append(product * (1.0 / scale))
    return rows


def cos_sin(phase):
    turns = jnp.floor(phase * (1.0 / math.pi) + 0.5)
    odd = turns - 2.0 * jnp.floor(turns * 0.5)
    sign = 1.0 - 2.0 * odd
    high = 3.140625
    rest = (phase - turns * high) - turns * (math.pi - high)
    square = rest * rest
    cosine = jnp.full_like(rest, 1.0 / math.factorial(12))
    for order in (10, 8, 6, 4, 2, 0):
        cosine = cosine * square + (1.0 if order % 4 == 0 else -1.0) / math.factorial(order)
    sine = jnp.full_like(rest, -1.0 / math.factorial(11))
    for order in (9, 7, 5, 3, 1):
        sine = sine * square + (1.0 if order % 4 == 1 else -1.0) / math.factorial(order)
    return cosine * sign, sine * rest * sign


def xor_pairs(count, bit):
    return [(i, i ^ (1 << bit)) for i in range(count)]


def log2(count):
    bits = count.bit_length() - 1
    if count != 1 << bits:
        raise ValueError("axis size")
    return bits


def spread(value, axis, bits):
    held = [value]
    count = lax.axis_size(axis)
    for bit in bits:
        held = held + [lax.ppermute(h, axis, xor_pairs(count, bit)) for h in held]
    return held


def block_sums(waves, numbers, places, blocks, previous, slot_count, cone_count):
    last = previous is not None
    units = 2 * cone_count
    lists = len(blocks)
    per_list, block_size, columns = blocks[0].shape
    total = lists * per_list
    height = units * SQUARE
    firsts = units * NODES
    rows = PLANE + firsts
    group = 16
    place_rows = 8
    half = slot_count // 2
    parents = LEAVES_DEV // OCTANTS

    def kernel(*refs):
        wave_ref = refs[0]
        number_refs = refs[1 : 1 + lists]
        place_refs = refs[1 + lists : 1 + 2 * lists]
        block_refs = refs[1 + 2 * lists : 1 + 3 * lists]
        at = 1 + 3 * lists
        if last:
            before_ref, keep_ref, send_ref, sum_ref = refs[at : at + 4]
        else:
            sum_ref = refs[at]
        factor_ref, place_ref, number_ref = refs[-3:]

        for which in range(lists):

            def unpack(index, carry):
                at_block = which * per_list + index
                place = place_refs[which][index].astype(jnp.float32)
                place_ref[pl.ds(pl.multiple_of(at_block * place_rows, place_rows), 3), :] = place
                leaf = number_refs[which][0, index]
                shifts = [(leaf >> 2) & 1, (leaf >> 1) & 1, leaf & 1]
                values = [(2 * shift - 1).astype(jnp.float32) for shift in shifts]
                values.append(number_refs[which][1, index].astype(jnp.float32))
                for row, value in enumerate(values):
                    number_ref[row, pl.ds(at_block, 1), :] = jnp.full(
                        (1, block_size), value, jnp.float32
                    )
                return carry

            lax.fori_loop(0, per_list, unpack, 0, unroll=4)

        lanes = lax.broadcasted_iota(jnp.int32, (group, block_size), 1).astype(jnp.float32)
        for part in range(total // group):
            span = pl.ds(part * group, group)
            double = [
                number_ref[d, span, :]
                + place_ref[pl.ds(part * group * place_rows + d, group, stride=place_rows), :]
                for d in range(3)
            ]
            live = lanes < number_ref[3, span, :]
            first = [jnp.where(live, r, 0.0) for r in lagrange_rows(0.5 * double[0])]
            second = lagrange_rows(0.5 * double[1])
            third = lagrange_rows(0.5 * double[2])
            start = part * group * rows

            def put(row, value):
                factor_ref[pl.ds(start + row, group, stride=rows), :] = value

            for a in range(NODES):
                for b in range(NODES):
                    put(a * NODES + b, second[a] * third[b])
            for cone in range(cone_count):
                phase = (
                    wave_ref[0, cone] * double[0]
                    + wave_ref[1, cone] * double[1]
                    + wave_ref[2, cone] * double[2]
                )
                cosine, sine = cos_sin(phase)
                for digit in range(NODES):
                    put(PLANE + cone * 2 * NODES + digit, first[digit] * cosine)
                    put(PLANE + cone * 2 * NODES + NODES + digit, first[digit] * -sine)

        sum_ref[...] = jnp.zeros_like(sum_ref)
        me = lax.axis_index("dom")
        bits = log2(lax.axis_size("dom"))

        def slot_of(which, index):
            leaf, owner = number_refs[which][0, index], number_refs[which][2, index]
            relative = owner ^ me
            order = leaf >> 3
            for bit in range(bits):
                order = order + (((relative >> bit) & 1) << (bits - 1 - bit)) * parents
            return order

        def weights_of(index):
            base = pl.multiple_of(index * rows, 8)
            pairs = factor_ref[pl.ds(base, PLANE), :]
            pieces = [
                (factor_ref[pl.ds(base + PLANE + row, 1), :] * pairs).astype(jnp.bfloat16)
                for row in range(firsts)
            ]
            return jnp.concatenate(pieces, axis=0)

        empty = jnp.zeros((block_size, columns), jnp.bfloat16)
        for which in range(lists):
            def two(pair, carry):
                index = which * per_list + 2 * pair
                weights = jnp.concatenate([weights_of(index), weights_of(index + 1)], axis=1)
                wide = jnp.concatenate(
                    [
                        jnp.concatenate([block_refs[which][2 * pair], empty], axis=1),
                        jnp.concatenate([empty, block_refs[which][2 * pair + 1]], axis=1),
                    ],
                    axis=0,
                )
                product = jnp.dot(weights, wide, preferred_element_type=jnp.float32)
                sum_ref[slot_of(which, 2 * pair)] += product[:, :columns]
                sum_ref[slot_of(which, 2 * pair + 1)] += product[:, columns:]
                return carry

            lax.fori_loop(0, per_list // 2, two, 0)

        if last:

            def finish(slot, carry):
                for unit in range(units):
                    span = pl.ds(unit * SQUARE, SQUARE)
                    keep_ref[unit, slot] = sum_ref[slot, span, :] + before_ref[slot, span, :]
                    send_ref[unit, slot] = (
                        sum_ref[half + slot, span, :] + before_ref[half + slot, span, :]
                    ).astype(jnp.bfloat16)
                return carry

            lax.fori_loop(0, half, finish, 0)

    whole = (slot_count, height, columns)
    scratch = [
        pltpu.VMEM((total * rows, block_size), jnp.float32),
        pltpu.VMEM((total * place_rows, block_size), jnp.float32),
        pltpu.VMEM((4, total, block_size), jnp.float32),
    ]
    out_shape = [jax.ShapeDtypeStruct(whole, jnp.float32)]
    if last:
        split = (units, half, SQUARE, columns)
        out_shape = [
            jax.ShapeDtypeStruct(split, jnp.float32),
            jax.ShapeDtypeStruct(split, jnp.bfloat16),
        ]
        scratch = [pltpu.VMEM(whole, jnp.float32)] + scratch
    operands = [waves, *numbers, *places, *blocks] + ([previous] if last else [])
    need = 3 * slot_count * height * columns * 4 + total * (rows + 12 + 64) * block_size * 4
    return pl.pallas_call(
        kernel,
        out_shape=out_shape,
        in_specs=[SMEM] * (1 + lists) + [VMEM] * (2 * lists + last),
        out_specs=[VMEM] * len(out_shape),
        scratch_shapes=scratch,
        compiler_params=pltpu.CompilerParams(vmem_limit_bytes=min(need + (3 << 20), 60 << 20)),
        cost_estimate=pl.CostEstimate(
            flops=2 * total * height * block_size * columns,
            bytes_accessed=total * block_size * columns * 2 + slot_count * height * columns * 4,
            transcendentals=0,
        ),
    )(*operands)


def rotate(sums, cone_waves):
    parents, units, square, columns = sums.shape
    cone_count = cone_waves.shape[1]
    digits = jnp.arange(square)
    digits = jnp.stack([digits // PLANE, digits // NODES % NODES, digits % NODES])
    nodes = jnp.cos((2.0 * digits.astype(jnp.float32) + 1.0) * (math.pi / (2.0 * NODES)))
    angle = 2.0 * (
        cone_waves[0][:, None] * nodes[0]
        + cone_waves[1][:, None] * nodes[1]
        + cone_waves[2][:, None] * nodes[2]
    )
    cosine, sine = jnp.cos(angle)[None, :, :, None], jnp.sin(angle)[None, :, :, None]
    parts = sums.reshape(parents, cone_count, 2, square, columns)
    real, imag = parts[:, :, 0], parts[:, :, 1]
    return jnp.stack([cosine * real - sine * imag, cosine * imag + sine * real], axis=2)


def mesh_flat():
    dirs = lax.axis_size("dir")
    return lax.axis_index("dom") * dirs + lax.axis_index("dir"), lax.axis_size("dom") * dirs


def greet_all():
    me, count = mesh_flat()
    dirs = lax.axis_size("dir")
    barrier = pltpu.get_barrier_semaphore()

    def one(offset, carry):
        peer = (me + offset) % count
        pl.semaphore_signal(
            barrier, inc=1, device_id=(peer // dirs, peer % dirs), device_id_type=MESH
        )
        return carry

    lax.fori_loop(1, count, one, 0)
    return barrier, count - 1


def send_rows(source, landing, width, send_sem, recv_sem):
    me, count = mesh_flat()
    dirs = lax.axis_size("dir")

    def one(offset, carry):
        peer = (me + offset) % count
        pltpu.make_async_remote_copy(
            src_ref=source.at[pl.ds(pl.multiple_of(peer * width, width), width)],
            dst_ref=landing.at[pl.ds(pl.multiple_of(me * width, width), width)],
            send_sem=send_sem,
            recv_sem=recv_sem,
            device_id=(peer // dirs, peer % dirs),
            device_id_type=MESH,
        ).start()
        return carry

    lax.fori_loop(1, count, one, 0)
    span = pl.ds(0, (count - 1) * width)
    peer = (me + 1) % count
    return pltpu.make_async_remote_copy(
        src_ref=source.at[span],
        dst_ref=landing.at[span],
        send_sem=send_sem,
        recv_sem=recv_sem,
        device_id=(peer // dirs, peer % dirs),
        device_id_type=MESH,
    )


def halo_rows(x_edges, send_list):
    owned_rows, columns = x_edges.shape
    partitions, width = send_list.shape

    def kernel(list_ref, x_ref, out_ref, table_ref, got_ref, send_ref, send_sem, recv_sem):
        barrier, others = greet_all()
        me, _ = mesh_flat()
        table_ref[...] = x_ref[...].astype(jnp.float32)

        def one(part, carry):
            start = pl.multiple_of(part * width, width)
            for lane in range(width):
                row = jnp.minimum(list_ref[part, lane], owned_rows - 1)
                got_ref[pl.ds(start + lane, 1), :] = table_ref[pl.ds(row, 1), :]
            return carry

        lax.fori_loop(0, partitions, one, 0)
        send_ref[...] = got_ref[...].astype(jnp.bfloat16)
        own = pl.ds(pl.multiple_of(me * width, width), width)
        out_ref[own, :] = jnp.zeros((width, columns), jnp.bfloat16)
        pl.semaphore_wait(barrier, others)
        whole = send_rows(send_ref, out_ref, width, send_sem, recv_sem)
        whole.wait_send()
        whole.wait_recv()

    return pl.pallas_call(
        kernel,
        out_shape=jax.ShapeDtypeStruct((partitions * width, columns), jnp.bfloat16),
        in_specs=[SMEM, VMEM],
        out_specs=VMEM,
        scratch_shapes=[
            pltpu.VMEM((owned_rows, columns), jnp.float32),
            pltpu.VMEM((partitions * width, columns), jnp.float32),
            pltpu.VMEM((partitions * width, columns), jnp.bfloat16),
            pltpu.SemaphoreType.DMA,
            pltpu.SemaphoreType.DMA,
        ],
        compiler_params=pltpu.CompilerParams(
            collective_id=0, has_side_effects=True, vmem_limit_bytes=16 << 20
        ),
        cost_estimate=pl.CostEstimate(
            flops=1_000_000_000, bytes_accessed=owned_rows * columns * 2, transcendentals=0
        ),
    )(send_list, x_edges)


def element_sums(links, live, x_edges, received, mats):
    element_count = mats.shape[1]
    edges = links.shape[0] // element_count
    owned_rows, columns = x_edges.shape
    halo = received.shape[0]
    table_rows = owned_rows + halo
    step = 8
    wide = 128

    def kernel(link_ref, live_ref, x_ref, halo_ref, mat_ref, own_ref, back_ref, *scratch):
        table_ref, term_ref = scratch[:2]
        got_refs, sums = scratch[2:4], scratch[4:]
        table_ref[pl.ds(0, owned_rows), :] = x_ref[...].astype(jnp.float32)
        table_ref[pl.ds(owned_rows, halo), :] = halo_ref[...].astype(jnp.float32)
        for ref in sums:
            ref[...] = jnp.zeros_like(ref)
        here = lax.broadcasted_iota(jnp.int32, (wide, wide), 0)
        there = lax.broadcasted_iota(jnp.int32, (wide, wide), 1)
        eye = jnp.where(here == there, 1.0, 0.0).astype(jnp.bfloat16)

        def fetch(number, got_ref):
            start = pl.multiple_of(number * wide, wide)
            for edge in range(edges):
                for lane in range(wide):
                    row = link_ref[start + (edge * element_count + lane)]
                    got_ref[pl.ds(edge * wide + lane, 1), :] = table_ref[pl.ds(row, 1), :]

        def product(number, got_ref):
            start = pl.multiple_of(number * wide, wide)
            count = start + lax.broadcasted_iota(jnp.int32, (1, wide), 1)
            live = count < live_ref[0]
            got = got_ref[...].astype(jnp.bfloat16)
            for i in range(edges):
                diagonals = []
                for j in range(edges):
                    row = mat_ref[pl.ds(edges * i + j, 1), pl.ds(start, wide)]
                    row = jnp.where(live, row, 0.0).astype(jnp.bfloat16)
                    diagonals.append(eye * row)
                term_ref[i, pl.ds(start, wide), :] = jnp.dot(
                    jnp.concatenate(diagonals, axis=1), got, preferred_element_type=jnp.float32
                )

        tiles = element_count // wide

        def products(index, carry):
            fetch(2 * index + 1, got_refs[1])
            product(2 * index, got_refs[0])
            fetch(jnp.minimum(2 * index + 2, tiles - 1), got_refs[0])
            product(2 * index + 1, got_refs[1])
            return carry

        fetch(0, got_refs[0])
        lax.fori_loop(0, tiles // 2, products, 0)

        def scatter(number, carry):
            start = pl.multiple_of(number * step, step)
            for lane in range(step):
                for edge in range(edges):
                    row = link_ref[start + (edge * element_count + lane)]
                    sums[edge][pl.ds(row, 1), :] += term_ref[edge, pl.ds(start + lane, 1), :]
            return carry

        lax.fori_loop(0, element_count // step, scatter, 0, unroll=2)

        def total_of(span):
            total = sums[0][span, :]
            for ref in sums[1:]:
                total = total + ref[span, :]
            return total

        own_ref[...] = total_of(pl.ds(0, owned_rows))
        back_ref[...] = total_of(pl.ds(owned_rows, halo)).astype(jnp.bfloat16)

    need = (edges + 4) * table_rows * columns * 4 + (6 << 20)
    return pl.pallas_call(
        kernel,
        out_shape=[
            jax.ShapeDtypeStruct((owned_rows, columns), jnp.float32),
            jax.ShapeDtypeStruct((halo, columns), jnp.bfloat16),
        ],
        in_specs=[SMEM, SMEM, VMEM, VMEM, VMEM],
        out_specs=[VMEM, VMEM],
        scratch_shapes=[
            pltpu.VMEM((table_rows, columns), jnp.float32),
            pltpu.VMEM((edges, element_count, columns), jnp.float32),
            pltpu.VMEM((edges * wide, columns), jnp.float32),
            pltpu.VMEM((edges * wide, columns), jnp.float32),
        ]
        + [pltpu.VMEM((table_rows, columns), jnp.float32)] * edges,
        compiler_params=pltpu.CompilerParams(vmem_limit_bytes=need),
        cost_estimate=pl.CostEstimate(
            flops=4_000_000_000, bytes_accessed=table_rows * columns * 8, transcendentals=0
        ),
    )(links, live, x_edges, received, mats)


def return_and_reduce(back, rows, keep, send, owned_rows, parents):
    partitions = lax.axis_size("dom") * lax.axis_size("dir")
    total_rows, columns = back.shape
    width = total_rows // partitions
    units, half, height, _ = keep.shape
    steps = log2(lax.axis_size("dom"))
    sizes = [half >> k for k in range(steps)]
    fold_step = 256

    def kernel(row_ref, back_ref, keep_ref, send_ref, fold_ref, out_ref, *scratch):
        land_ref = scratch[0]
        got = scratch[1 : 1 + steps]
        keeps = [keep_ref] + list(scratch[1 + steps : 2 * steps])
        sends = [send_ref] + list(scratch[2 * steps : 3 * steps - 1])
        back_send, back_recv, send_sems, recv_sems = scratch[3 * steps - 1 :]
        me, _ = mesh_flat()
        dom = lax.axis_index("dom")
        barrier, others = greet_all()
        own = pl.ds(pl.multiple_of(me * width, width), width)
        land_ref[own, :] = jnp.zeros((width, columns), jnp.bfloat16)
        pl.semaphore_wait(barrier, others)
        def copy(k, unit):
            bit = 1 << k
            partner = dom + bit * (1 - 2 * ((dom // bit) % 2))
            return pltpu.make_async_remote_copy(
                src_ref=sends[k].at[unit],
                dst_ref=got[k].at[unit],
                send_sem=send_sems.at[k, unit],
                recv_sem=recv_sems.at[k, unit],
                device_id=(partner, lax.axis_index("dir")),
                device_id_type=MESH,
            )

        for unit in range(units):
            copy(0, unit).start()
        whole = send_rows(back_ref, land_ref, width, back_send, back_recv)

        def fold_all():
            whole.wait_recv()
            landed = land_ref[...]
            listed = row_ref[...]

            def fold(index, carry):
                start = pl.multiple_of(index * fold_step, fold_step)
                mine = start + lax.broadcasted_iota(jnp.int32, (fold_step, total_rows), 0)
                picks = jnp.where(mine == listed, 1.0, 0.0).astype(jnp.bfloat16)
                fold_ref[pl.ds(start, fold_step), :] = jnp.dot(
                    picks, landed, preferred_element_type=jnp.float32
                )
                return carry

            lax.fori_loop(0, owned_rows // fold_step, fold, 0)

        for turn in range(units + steps - 1):
            if turn == units:
                fold_all()
            for k in range(steps):
                unit = turn - k
                if not 0 <= unit < units:
                    continue
                copy(k, unit).wait_recv()
                if k < steps - 1:
                    low = sizes[k + 1]
                    upper, lower = pl.ds(low, low), pl.ds(0, low)
                    sends[k + 1][unit] = (
                        keeps[k][unit, upper] + got[k][unit, upper].astype(jnp.float32)
                    ).astype(jnp.bfloat16)
                    copy(k + 1, unit).start()
                    keeps[k + 1][unit] = keeps[k][unit, lower] + got[k][unit, lower].astype(
                        jnp.float32
                    )
                else:
                    for parent in range(parents):
                        out_ref[parent, unit] = keeps[k][unit, parent] + got[k][
                            unit, parent
                        ].astype(jnp.float32)
        whole.wait_send()
        for k in range(steps):
            for unit in range(units):
                copy(k, unit).wait_send()

    def buffers(dtype, first):
        return [pltpu.VMEM((units, size, height, columns), dtype) for size in sizes[first:]]

    scratch = (
        [pltpu.VMEM((total_rows, columns), jnp.bfloat16)]
        + buffers(jnp.bfloat16, 0)
        + buffers(jnp.float32, 1)
        + buffers(jnp.bfloat16, 1)
    )
    need = half * units * height * columns * 16 + total_rows * columns * 16 + (8 << 20)
    return pl.pallas_call(
        kernel,
        out_shape=[
            jax.ShapeDtypeStruct((owned_rows, columns), jnp.float32),
            jax.ShapeDtypeStruct((parents, units, height, columns), jnp.float32),
        ],
        in_specs=[VMEM] * 4,
        out_specs=[VMEM, VMEM],
        scratch_shapes=scratch
        + [
            pltpu.SemaphoreType.DMA,
            pltpu.SemaphoreType.DMA,
            pltpu.SemaphoreType.DMA((steps, units)),
            pltpu.SemaphoreType.DMA((steps, units)),
        ],
        compiler_params=pltpu.CompilerParams(
            collective_id=1, has_side_effects=True, vmem_limit_bytes=min(need, 60 << 20)
        ),
        cost_estimate=pl.CostEstimate(
            flops=2 * owned_rows * total_rows * columns,
            bytes_accessed=half * units * height * columns * 6,
            transcendentals=0,
        ),
    )(rows, back, keep, send)


def shards(
    x_edges,
    send_list,
    connectivity,
    elem_mats,
    elem_live,
    currents,
    positions,
    block_live,
    block_owner,
    block_leaf,
    cone_waves,
):
    dom_count, dir_count = lax.axis_size("dom"), lax.axis_size("dir")
    parents = LEAVES_DEV // OCTANTS
    slot_count = dom_count * parents
    dir_bits = log2(dir_count)
    cone_count = cone_waves.shape[1]
    owned_rows = x_edges.shape[0]

    numbers = jnp.stack([block_leaf, block_live, block_owner])
    own = (numbers, positions, currents)
    near_bits = list(range(dir_bits - 1))
    near = [spread(value, "dir", near_bits) for value in own]
    received = halo_rows(x_edges, send_list)
    late, received = lax.optimization_barrier((currents, received))
    own = (numbers, positions, late)
    far = [lax.ppermute(value, "dir", xor_pairs(dir_count, dir_bits - 1)) for value in own]
    owned, back = element_sums(connectivity.reshape(-1), elem_live, x_edges, received, elem_mats)
    (sums,) = block_sums(cone_waves, *near, None, slot_count, cone_count)
    *far, back = lax.optimization_barrier((*far, back))
    far = [spread(value, "dir", near_bits) for value in far]
    keep, send = block_sums(cone_waves, *far, sums, slot_count, cone_count)
    fold, sums = return_and_reduce(
        back, send_list.reshape(1, -1), keep, send, owned_rows, parents
    )
    return owned + fold, rotate(sums, cone_waves)


def solution(mesh):
    placed = (
        P(("dom", "dir"), None),
        P(("dom", "dir"), None),
        P(None, ("dom", "dir")),
        P(None, ("dom", "dir")),
        P(("dom", "dir")),
        P(("dom", "dir"), None, None),
        P(("dom", "dir"), None, None),
        P(("dom", "dir")),
        P(("dom", "dir")),
        P(("dom", "dir")),
        P(None, "dir"),
    )
    return jax.shard_map(
        shards,
        mesh=mesh,
        in_specs=placed,
        out_specs=(P(("dom", "dir"), None), P("dom", "dir", None, None, None)),
        check_vma=False,
    )
```

```python
import math

import jax
import jax.numpy as jnp
from jax import lax
from jax.experimental import pallas as pl
from jax.experimental.pallas import tpu as pltpu
from jax.sharding import PartitionSpec as P

LEAVES_DEV = 16
OCTANTS = 8
NODES = 4
PLANE = NODES * NODES
SQUARE = NODES**3
POINTS = [math.cos((2 * j + 1) * math.pi / (2 * NODES)) for j in range(NODES)]
MESH = pl.DeviceIdType.MESH
VMEM = pl.BlockSpec(memory_space=pltpu.VMEM)
SMEM = pl.BlockSpec(memory_space=pltpu.SMEM)


def lagrange_rows(v):
    rows = []
    for target in range(NODES):
        product = None
        scale = 1.0
        for other in range(NODES):
            if other != target:
                factor = v - POINTS[other]
                product = factor if product is None else product * factor
                scale *= POINTS[target] - POINTS[other]
        rows.append(product * (1.0 / scale))
    return rows


def cos_sin(phase):
    turns = jnp.floor(phase * (1.0 / math.pi) + 0.5)
    odd = turns - 2.0 * jnp.floor(turns * 0.5)
    sign = 1.0 - 2.0 * odd
    high = 3.140625
    rest = (phase - turns * high) - turns * (math.pi - high)
    square = rest * rest
    cosine = jnp.full_like(rest, 1.0 / math.factorial(12))
    for order in (10, 8, 6, 4, 2, 0):
        cosine = cosine * square + (1.0 if order % 4 == 0 else -1.0) / math.factorial(order)
    sine = jnp.full_like(rest, -1.0 / math.factorial(11))
    for order in (9, 7, 5, 3, 1):
        sine = sine * square + (1.0 if order % 4 == 1 else -1.0) / math.factorial(order)
    return cosine * sign, sine * rest * sign


def xor_pairs(count, bit):
    return [(i, i ^ (1 << bit)) for i in range(count)]


def log2(count):
    bits = count.bit_length() - 1
    if count != 1 << bits:
        raise ValueError("axis size")
    return bits


def spread(value, axis, bits):
    held = [value]
    count = lax.axis_size(axis)
    for bit in bits:
        held = held + [lax.ppermute(h, axis, xor_pairs(count, bit)) for h in held]
    return held


def block_sums(waves, numbers, places, blocks, previous, slot_count, cone_count):
    last = previous is not None
    units = 2 * cone_count
    lists = len(blocks)
    per_list, block_size, columns = blocks[0].shape
    total = lists * per_list
    height = units * SQUARE
    firsts = units * NODES
    rows = PLANE + firsts + 8
    group = 16
    place_rows = 8
    half = slot_count // 2
    parents = LEAVES_DEV // OCTANTS

    def kernel(*refs):
        wave_ref = refs[0]
        number_refs = refs[1 : 1 + lists]
        place_refs = refs[1 + lists : 1 + 2 * lists]
        block_refs = refs[1 + 2 * lists : 1 + 3 * lists]
        at = 1 + 3 * lists
        if last:
            before_ref, keep_ref, send_ref, sum_ref = refs[at : at + 4]
        else:
            sum_ref = refs[at]
        factor_ref, place_ref, number_ref = refs[-3:]

        for which in range(lists):

            def unpack(index, carry):
                at_block = which * per_list + index
                place = place_refs[which][index].astype(jnp.float32)
                place_ref[pl.ds(pl.multiple_of(at_block * place_rows, place_rows), 3), :] = place
                leaf = number_refs[which][0, index]
                shifts = [(leaf >> 2) & 1, (leaf >> 1) & 1, leaf & 1]
                values = [(2 * shift - 1).astype(jnp.float32) for shift in shifts]
                values.append(number_refs[which][1, index].astype(jnp.float32))
                for row, value in enumerate(values):
                    number_ref[row, pl.ds(at_block, 1), :] = jnp.full(
                        (1, block_size), value, jnp.float32
                    )
                return carry

            lax.fori_loop(0, per_list, unpack, 0, unroll=4)

        lanes = lax.broadcasted_iota(jnp.int32, (group, block_size), 1).astype(jnp.float32)
        for part in range(total // group):
            span = pl.ds(part * group, group)
            double = [
                number_ref[d, span, :]
                + place_ref[pl.ds(part * group * place_rows + d, group, stride=place_rows), :]
                for d in range(3)
            ]
            live = lanes < number_ref[3, span, :]
            first = [jnp.where(live, r, 0.0) for r in lagrange_rows(0.5 * double[0])]
            second = lagrange_rows(0.5 * double[1])
            third = lagrange_rows(0.5 * double[2])
            start = part * group * rows

            def put(row, value):
                factor_ref[pl.ds(start + row, group, stride=rows), :] = value

            for a in range(NODES):
                for b in range(NODES):
                    put(a * NODES + b, second[a] * third[b])
            for cone in range(cone_count):
                phase = (
                    wave_ref[0, cone] * double[0]
                    + wave_ref[1, cone] * double[1]
                    + wave_ref[2, cone] * double[2]
                )
                cosine, sine = cos_sin(phase)
                for digit in range(NODES):
                    put(PLANE + cone * 2 * NODES + digit, first[digit] * cosine)
                    put(PLANE + cone * 2 * NODES + NODES + digit, first[digit] * -sine)

        sum_ref[...] = jnp.zeros_like(sum_ref)
        me = lax.axis_index("dom")
        bits = log2(lax.axis_size("dom"))

        def slot_of(which, index):
            leaf, owner = number_refs[which][0, index], number_refs[which][2, index]
            relative = owner ^ me
            order = leaf >> 3
            for bit in range(bits):
                order = order + (((relative >> bit) & 1) << (bits - 1 - bit)) * parents
            return order

        def weights_of(index):
            base = pl.multiple_of(index * rows, 8)
            pairs = factor_ref[pl.ds(base, PLANE), :]
            pieces = [
                (factor_ref[pl.ds(base + PLANE + row, 1), :] * pairs).astype(jnp.bfloat16)
                for row in range(firsts)
            ]
            return jnp.concatenate(pieces, axis=0)

        for which in range(lists):

            def one(index, carry):
                product = jnp.dot(
                    weights_of(which * per_list + index),
                    block_refs[which][index],
                    preferred_element_type=jnp.float32,
                )
                sum_ref[slot_of(which, index)] += product
                return carry

            lax.fori_loop(0, per_list, one, 0, unroll=8)

        if last:

            def finish(slot, carry):
                for unit in range(units):
                    span = pl.ds(unit * SQUARE, SQUARE)
                    keep_ref[unit, slot] = sum_ref[slot, span, :] + before_ref[slot, span, :]
                    send_ref[unit, slot] = (
                        sum_ref[half + slot, span, :] + before_ref[half + slot, span, :]
                    ).astype(jnp.bfloat16)
                return carry

            lax.fori_loop(0, half, finish, 0)

    whole = (slot_count, height, columns)
    scratch = [
        pltpu.VMEM((total * rows, block_size), jnp.float32),
        pltpu.VMEM((total * place_rows, block_size), jnp.float32),
        pltpu.VMEM((4, total, block_size), jnp.float32),
    ]
    out_shape = [jax.ShapeDtypeStruct(whole, jnp.float32)]
    if last:
        split = (units, half, SQUARE, columns)
        out_shape = [
            jax.ShapeDtypeStruct(split, jnp.float32),
            jax.ShapeDtypeStruct(split, jnp.bfloat16),
        ]
        scratch = [pltpu.VMEM(whole, jnp.float32)] + scratch
    operands = [waves, *numbers, *places, *blocks] + ([previous] if last else [])
    need = 3 * slot_count * height * columns * 4 + total * (rows + 12 + 64) * block_size * 4
    return pl.pallas_call(
        kernel,
        out_shape=out_shape,
        in_specs=[SMEM] * (1 + lists) + [VMEM] * (2 * lists + last),
        out_specs=[VMEM] * len(out_shape),
        scratch_shapes=scratch,
        compiler_params=pltpu.CompilerParams(vmem_limit_bytes=min(need + (3 << 20), 60 << 20)),
        cost_estimate=pl.CostEstimate(
            flops=2 * total * height * block_size * columns,
            bytes_accessed=total * block_size * columns * 2 + slot_count * height * columns * 4,
            transcendentals=0,
        ),
    )(*operands)


def rotate(sums, cone_waves):
    parents, units, square, columns = sums.shape
    cone_count = cone_waves.shape[1]
    digits = jnp.arange(square)
    digits = jnp.stack([digits // PLANE, digits // NODES % NODES, digits % NODES])
    nodes = jnp.cos((2.0 * digits.astype(jnp.float32) + 1.0) * (math.pi / (2.0 * NODES)))
    angle = 2.0 * (
        cone_waves[0][:, None] * nodes[0]
        + cone_waves[1][:, None] * nodes[1]
        + cone_waves[2][:, None] * nodes[2]
    )
    cosine, sine = jnp.cos(angle)[None, :, :, None], jnp.sin(angle)[None, :, :, None]
    parts = sums.reshape(parents, cone_count, 2, square, columns)
    real, imag = parts[:, :, 0], parts[:, :, 1]
    return jnp.stack([cosine * real - sine * imag, cosine * imag + sine * real], axis=2)


def mesh_flat():
    dirs = lax.axis_size("dir")
    return lax.axis_index("dom") * dirs + lax.axis_index("dir"), lax.axis_size("dom") * dirs


def greet_all():
    me, count = mesh_flat()
    dirs = lax.axis_size("dir")
    barrier = pltpu.get_barrier_semaphore()

    def one(offset, carry):
        peer = (me + offset) % count
        pl.semaphore_signal(
            barrier, inc=1, device_id=(peer // dirs, peer % dirs), device_id_type=MESH
        )
        return carry

    lax.fori_loop(1, count, one, 0)
    return barrier, count - 1


def send_rows(source, landing, width, send_sem, recv_sem):
    me, count = mesh_flat()
    dirs = lax.axis_size("dir")

    def one(offset, carry):
        peer = (me + offset) % count
        pltpu.make_async_remote_copy(
            src_ref=source.at[pl.ds(pl.multiple_of(peer * width, width), width)],
            dst_ref=landing.at[pl.ds(pl.multiple_of(me * width, width), width)],
            send_sem=send_sem,
            recv_sem=recv_sem,
            device_id=(peer // dirs, peer % dirs),
            device_id_type=MESH,
        ).start()
        return carry

    lax.fori_loop(1, count, one, 0)
    span = pl.ds(0, (count - 1) * width)
    peer = (me + 1) % count
    return pltpu.make_async_remote_copy(
        src_ref=source.at[span],
        dst_ref=landing.at[span],
        send_sem=send_sem,
        recv_sem=recv_sem,
        device_id=(peer // dirs, peer % dirs),
        device_id_type=MESH,
    )


def halo_rows(x_edges, send_list):
    owned_rows, columns = x_edges.shape
    partitions, width = send_list.shape

    def kernel(list_ref, x_ref, out_ref, table_ref, got_ref, send_ref, send_sem, recv_sem):
        barrier, others = greet_all()
        me, _ = mesh_flat()
        table_ref[...] = x_ref[...].astype(jnp.float32)

        def one(part, carry):
            start = pl.multiple_of(part * width, width)
            for lane in range(width):
                row = jnp.minimum(list_ref[part, lane], owned_rows - 1)
                got_ref[pl.ds(start + lane, 1), :] = table_ref[pl.ds(row, 1), :]
            return carry

        lax.fori_loop(0, partitions, one, 0)
        send_ref[...] = got_ref[...].astype(jnp.bfloat16)
        own = pl.ds(pl.multiple_of(me * width, width), width)
        out_ref[own, :] = jnp.zeros((width, columns), jnp.bfloat16)
        pl.semaphore_wait(barrier, others)
        whole = send_rows(send_ref, out_ref, width, send_sem, recv_sem)
        whole.wait_send()
        whole.wait_recv()

    return pl.pallas_call(
        kernel,
        out_shape=jax.ShapeDtypeStruct((partitions * width, columns), jnp.bfloat16),
        in_specs=[SMEM, VMEM],
        out_specs=VMEM,
        scratch_shapes=[
            pltpu.VMEM((owned_rows, columns), jnp.float32),
            pltpu.VMEM((partitions * width, columns), jnp.float32),
            pltpu.VMEM((partitions * width, columns), jnp.bfloat16),
            pltpu.SemaphoreType.DMA,
            pltpu.SemaphoreType.DMA,
        ],
        compiler_params=pltpu.CompilerParams(
            collective_id=0, has_side_effects=True, vmem_limit_bytes=16 << 20
        ),
        cost_estimate=pl.CostEstimate(
            flops=1_000_000_000, bytes_accessed=owned_rows * columns * 2, transcendentals=0
        ),
    )(send_list, x_edges)


def element_sums(links, live, x_edges, received, mats):
    element_count = mats.shape[1]
    edges = links.shape[0] // element_count
    owned_rows, columns = x_edges.shape
    halo = received.shape[0]
    table_rows = owned_rows + halo
    step = 8
    wide = 128

    def kernel(link_ref, live_ref, x_ref, halo_ref, mat_ref, own_ref, back_ref, *scratch):
        table_ref, term_ref = scratch[:2]
        got_refs, sums = scratch[2:4], scratch[4:]
        table_ref[pl.ds(0, owned_rows), :] = x_ref[...].astype(jnp.float32)
        table_ref[pl.ds(owned_rows, halo), :] = halo_ref[...].astype(jnp.float32)
        for ref in sums:
            ref[...] = jnp.zeros_like(ref)
        here = lax.broadcasted_iota(jnp.int32, (wide, wide), 0)
        there = lax.broadcasted_iota(jnp.int32, (wide, wide), 1)
        eye = jnp.where(here == there, 1.0, 0.0).astype(jnp.bfloat16)

        def fetch(number, got_ref):
            start = pl.multiple_of(number * wide, wide)
            for edge in range(edges):
                for lane in range(wide):
                    row = link_ref[start + (edge * element_count + lane)]
                    got_ref[pl.ds(edge * wide + lane, 1), :] = table_ref[pl.ds(row, 1), :]

        def product(number, got_ref):
            start = pl.multiple_of(number * wide, wide)
            count = start + lax.broadcasted_iota(jnp.int32, (1, wide), 1)
            live = count < live_ref[0]
            got = got_ref[...].astype(jnp.bfloat16)
            for i in range(edges):
                diagonals = []
                for j in range(edges):
                    row = mat_ref[pl.ds(edges * i + j, 1), pl.ds(start, wide)]
                    row = jnp.where(live, row, 0.0).astype(jnp.bfloat16)
                    diagonals.append(eye * row)
                term_ref[i, pl.ds(start, wide), :] = jnp.dot(
                    jnp.concatenate(diagonals, axis=1), got, preferred_element_type=jnp.float32
                )

        tiles = element_count // wide

        def products(index, carry):
            fetch(2 * index + 1, got_refs[1])
            product(2 * index, got_refs[0])
            fetch(jnp.minimum(2 * index + 2, tiles - 1), got_refs[0])
            product(2 * index + 1, got_refs[1])
            return carry

        fetch(0, got_refs[0])
        lax.fori_loop(0, tiles // 2, products, 0)

        def scatter(number, carry):
            start = pl.multiple_of(number * step, step)
            for lane in range(step):
                for edge in range(edges):
                    row = link_ref[start + (edge * element_count + lane)]
                    sums[edge][pl.ds(row, 1), :] += term_ref[edge, pl.ds(start + lane, 1), :]
            return carry

        lax.fori_loop(0, element_count // step, scatter, 0, unroll=2)

        def total_of(span):
            total = sums[0][span, :]
            for ref in sums[1:]:
                total = total + ref[span, :]
            return total

        own_ref[...] = total_of(pl.ds(0, owned_rows))
        back_ref[...] = total_of(pl.ds(owned_rows, halo)).astype(jnp.bfloat16)

    need = (edges + 4) * table_rows * columns * 4 + (6 << 20)
    return pl.pallas_call(
        kernel,
        out_shape=[
            jax.ShapeDtypeStruct((owned_rows, columns), jnp.float32),
            jax.ShapeDtypeStruct((halo, columns), jnp.bfloat16),
        ],
        in_specs=[SMEM, SMEM, VMEM, VMEM, VMEM],
        out_specs=[VMEM, VMEM],
        scratch_shapes=[
            pltpu.VMEM((table_rows, columns), jnp.float32),
            pltpu.VMEM((edges, element_count, columns), jnp.float32),
            pltpu.VMEM((edges * wide, columns), jnp.float32),
            pltpu.VMEM((edges * wide, columns), jnp.float32),
        ]
        + [pltpu.VMEM((table_rows, columns), jnp.float32)] * edges,
        compiler_params=pltpu.CompilerParams(vmem_limit_bytes=need),
        cost_estimate=pl.CostEstimate(
            flops=4_000_000_000, bytes_accessed=table_rows * columns * 8, transcendentals=0
        ),
    )(links, live, x_edges, received, mats)


def return_and_reduce(back, rows, keep, send, owned_rows, parents):
    partitions = lax.axis_size("dom") * lax.axis_size("dir")
    total_rows, columns = back.shape
    width = total_rows // partitions
    units, half, height, _ = keep.shape
    steps = log2(lax.axis_size("dom"))
    sizes = [half >> k for k in range(steps)]
    fold_step = 256
    lag = 2

    def kernel(row_ref, back_ref, keep_ref, send_ref, fold_ref, out_ref, *scratch):
        land_ref = scratch[0]
        got = scratch[1 : 1 + steps]
        keeps = [keep_ref] + list(scratch[1 + steps : 2 * steps])
        sends = [send_ref] + list(scratch[2 * steps : 3 * steps - 1])
        back_send, back_recv, send_sems, recv_sems = scratch[3 * steps - 1 :]
        me, _ = mesh_flat()
        dom = lax.axis_index("dom")
        barrier, others = greet_all()
        own = pl.ds(pl.multiple_of(me * width, width), width)
        land_ref[own, :] = jnp.zeros((width, columns), jnp.bfloat16)
        pl.semaphore_wait(barrier, others)
        def copy(k, unit):
            bit = 1 << k
            partner = dom + bit * (1 - 2 * ((dom // bit) % 2))
            return pltpu.make_async_remote_copy(
                src_ref=sends[k].at[unit],
                dst_ref=got[k].at[unit],
                send_sem=send_sems.at[k, unit],
                recv_sem=recv_sems.at[k, unit],
                device_id=(partner, lax.axis_index("dir")),
                device_id_type=MESH,
            )

        for unit in range(units):
            copy(0, unit).start()
        whole = send_rows(back_ref, land_ref, width, back_send, back_recv)

        def fold_all():
            whole.wait_recv()
            landed = land_ref[...]
            listed = row_ref[...]

            def fold(index, carry):
                start = pl.multiple_of(index * fold_step, fold_step)
                mine = start + lax.broadcasted_iota(jnp.int32, (fold_step, total_rows), 0)
                picks = jnp.where(mine == listed, 1.0, 0.0).astype(jnp.bfloat16)
                fold_ref[pl.ds(start, fold_step), :] = jnp.dot(
                    picks, landed, preferred_element_type=jnp.float32
                )
                return carry

            lax.fori_loop(0, owned_rows // fold_step, fold, 0)

        for turn in range(units + lag * (steps - 1)):
            for k in reversed(range(steps)):
                unit = turn - lag * k
                if not 0 <= unit < units:
                    continue
                copy(k, unit).wait_recv()
                if k < steps - 1:
                    low = sizes[k + 1]
                    upper, lower = pl.ds(low, low), pl.ds(0, low)
                    sends[k + 1][unit] = (
                        keeps[k][unit, upper] + got[k][unit, upper].astype(jnp.float32)
                    ).astype(jnp.bfloat16)
                    copy(k + 1, unit).start()
                    keeps[k + 1][unit] = keeps[k][unit, lower] + got[k][unit, lower].astype(
                        jnp.float32
                    )
                else:
                    for parent in range(parents):
                        out_ref[parent, unit] = keeps[k][unit, parent] + got[k][
                            unit, parent
                        ].astype(jnp.float32)
            if turn == units - 1 + lag * (steps - 2):
                fold_all()
        whole.wait_send()
        for k in range(steps):
            for unit in range(units):
                copy(k, unit).wait_send()

    def buffers(dtype, first):
        return [pltpu.VMEM((units, size, height, columns), dtype) for size in sizes[first:]]

    scratch = (
        [pltpu.VMEM((total_rows, columns), jnp.bfloat16)]
        + buffers(jnp.bfloat16, 0)
        + buffers(jnp.float32, 1)
        + buffers(jnp.bfloat16, 1)
    )
    need = half * units * height * columns * 16 + total_rows * columns * 16 + (8 << 20)
    return pl.pallas_call(
        kernel,
        out_shape=[
            jax.ShapeDtypeStruct((owned_rows, columns), jnp.float32),
            jax.ShapeDtypeStruct((parents, units, height, columns), jnp.float32),
        ],
        in_specs=[VMEM] * 4,
        out_specs=[VMEM, VMEM],
        scratch_shapes=scratch
        + [
            pltpu.SemaphoreType.DMA,
            pltpu.SemaphoreType.DMA,
            pltpu.SemaphoreType.DMA((steps, units)),
            pltpu.SemaphoreType.DMA((steps, units)),
        ],
        compiler_params=pltpu.CompilerParams(
            collective_id=1, has_side_effects=True, vmem_limit_bytes=min(need, 60 << 20)
        ),
        cost_estimate=pl.CostEstimate(
            flops=2 * owned_rows * total_rows * columns,
            bytes_accessed=half * units * height * columns * 6,
            transcendentals=0,
        ),
    )(rows, back, keep, send)


def shards(
    x_edges,
    send_list,
    connectivity,
    elem_mats,
    elem_live,
    currents,
    positions,
    block_live,
    block_owner,
    block_leaf,
    cone_waves,
):
    dom_count, dir_count = lax.axis_size("dom"), lax.axis_size("dir")
    parents = LEAVES_DEV // OCTANTS
    slot_count = dom_count * parents
    dir_bits = log2(dir_count)
    cone_count = cone_waves.shape[1]
    owned_rows = x_edges.shape[0]

    numbers = jnp.stack([block_leaf, block_live, block_owner])
    own = (numbers, positions, currents)
    near_bits = list(range(dir_bits - 1))
    near = [spread(value, "dir", near_bits) for value in own]
    received = halo_rows(x_edges, send_list)
    late, received = lax.optimization_barrier((currents, received))
    own = (numbers, positions, late)
    far = [lax.ppermute(value, "dir", xor_pairs(dir_count, dir_bits - 1)) for value in own]
    owned, back = element_sums(connectivity.reshape(-1), elem_live, x_edges, received, elem_mats)
    (sums,) = block_sums(cone_waves, *near, None, slot_count, cone_count)
    *far, back = lax.optimization_barrier((*far, back))
    far = [spread(value, "dir", near_bits) for value in far]
    keep, send = block_sums(cone_waves, *far, sums, slot_count, cone_count)
    fold, sums = return_and_reduce(
        back, send_list.reshape(1, -1), keep, send, owned_rows, parents
    )
    return owned + fold, rotate(sums, cone_waves)


def solution(mesh):
    placed = (
        P(("dom", "dir"), None),
        P(("dom", "dir"), None),
        P(None, ("dom", "dir")),
        P(None, ("dom", "dir")),
        P(("dom", "dir")),
        P(("dom", "dir"), None, None),
        P(("dom", "dir"), None, None),
        P(("dom", "dir")),
        P(("dom", "dir")),
        P(("dom", "dir")),
        P(None, "dir"),
    )
    return jax.shard_map(
        shards,
        mesh=mesh,
        in_specs=placed,
        out_specs=(P(("dom", "dir"), None), P("dom", "dir", None, None, None)),
        check_vma=False,
    )
```

```python
import math

import jax
import jax.numpy as jnp
from jax import lax
from jax.experimental import pallas as pl
from jax.experimental.pallas import tpu as pltpu
from jax.sharding import PartitionSpec as P

LEAVES_DEV = 16
OCTANTS = 8
NODES = 4
PLANE = NODES * NODES
SQUARE = NODES**3
POINTS = [math.cos((2 * j + 1) * math.pi / (2 * NODES)) for j in range(NODES)]
MESH = pl.DeviceIdType.MESH
VMEM = pl.BlockSpec(memory_space=pltpu.VMEM)
SMEM = pl.BlockSpec(memory_space=pltpu.SMEM)


def lagrange_rows(v):
    rows = []
    for target in range(NODES):
        product = None
        scale = 1.0
        for other in range(NODES):
            if other != target:
                factor = v - POINTS[other]
                product = factor if product is None else product * factor
                scale *= POINTS[target] - POINTS[other]
        rows.append(product * (1.0 / scale))
    return rows


def cos_sin(phase):
    turns = jnp.floor(phase * (1.0 / math.pi) + 0.5)
    odd = turns - 2.0 * jnp.floor(turns * 0.5)
    sign = 1.0 - 2.0 * odd
    high = 3.140625
    rest = (phase - turns * high) - turns * (math.pi - high)
    square = rest * rest
    cosine = jnp.full_like(rest, 1.0 / math.factorial(12))
    for order in (10, 8, 6, 4, 2, 0):
        cosine = cosine * square + (1.0 if order % 4 == 0 else -1.0) / math.factorial(order)
    sine = jnp.full_like(rest, -1.0 / math.factorial(11))
    for order in (9, 7, 5, 3, 1):
        sine = sine * square + (1.0 if order % 4 == 1 else -1.0) / math.factorial(order)
    return cosine * sign, sine * rest * sign


def xor_pairs(count, bit):
    return [(i, i ^ (1 << bit)) for i in range(count)]


def log2(count):
    bits = count.bit_length() - 1
    if count != 1 << bits:
        raise ValueError("axis size")
    return bits


def turned_units(units):
    return units // 4


def spread(value, axis, bits):
    held = [value]
    count = lax.axis_size(axis)
    for bit in bits:
        held = held + [lax.ppermute(h, axis, xor_pairs(count, bit)) for h in held]
    return held


def block_sums(waves, numbers, places, blocks, previous, slot_count, cone_count):
    last = previous is not None
    units = 2 * cone_count
    lists = len(blocks)
    per_list, block_size, columns = blocks[0].shape
    total = lists * per_list
    height = units * SQUARE
    firsts = units * NODES
    rows = PLANE + firsts + 8
    group = 16
    place_rows = 8
    half = slot_count // 2
    parents = LEAVES_DEV // OCTANTS

    def kernel(*refs):
        wave_ref = refs[0]
        number_refs = refs[1 : 1 + lists]
        place_refs = refs[1 + lists : 1 + 2 * lists]
        block_refs = refs[1 + 2 * lists : 1 + 3 * lists]
        at = 1 + 3 * lists
        if last:
            before_ref, keep_ref, send_ref, sum_ref = refs[at : at + 4]
        else:
            sum_ref = refs[at]
        factor_ref, place_ref, number_ref = refs[-3:]

        for which in range(lists):

            def unpack(index, carry):
                at_block = which * per_list + index
                place = place_refs[which][index].astype(jnp.float32)
                place_ref[pl.ds(pl.multiple_of(at_block * place_rows, place_rows), 3), :] = place
                leaf = number_refs[which][0, index]
                shifts = [(leaf >> 2) & 1, (leaf >> 1) & 1, leaf & 1]
                values = [(2 * shift - 1).astype(jnp.float32) for shift in shifts]
                values.append(number_refs[which][1, index].astype(jnp.float32))
                for row, value in enumerate(values):
                    number_ref[row, pl.ds(at_block, 1), :] = jnp.full(
                        (1, block_size), value, jnp.float32
                    )
                return carry

            lax.fori_loop(0, per_list, unpack, 0, unroll=4)

        lanes = lax.broadcasted_iota(jnp.int32, (group, block_size), 1).astype(jnp.float32)
        for part in range(total // group):
            span = pl.ds(part * group, group)
            double = [
                number_ref[d, span, :]
                + place_ref[pl.ds(part * group * place_rows + d, group, stride=place_rows), :]
                for d in range(3)
            ]
            live = lanes < number_ref[3, span, :]
            first = [jnp.where(live, r, 0.0) for r in lagrange_rows(0.5 * double[0])]
            second = lagrange_rows(0.5 * double[1])
            third = lagrange_rows(0.5 * double[2])
            start = part * group * rows

            def put(row, value):
                factor_ref[pl.ds(start + row, group, stride=rows), :] = value

            for a in range(NODES):
                for b in range(NODES):
                    put(a * NODES + b, second[a] * third[b])
            for cone in range(cone_count):
                phase = (
                    wave_ref[0, cone] * double[0]
                    + wave_ref[1, cone] * double[1]
                    + wave_ref[2, cone] * double[2]
                )
                cosine, sine = cos_sin(phase)
                for digit in range(NODES):
                    put(PLANE + cone * 2 * NODES + digit, first[digit] * cosine)
                    put(PLANE + cone * 2 * NODES + NODES + digit, first[digit] * -sine)

        sum_ref[...] = jnp.zeros_like(sum_ref)
        me = lax.axis_index("dom")
        bits = log2(lax.axis_size("dom"))

        def slot_of(which, index):
            leaf, owner = number_refs[which][0, index], number_refs[which][2, index]
            relative = owner ^ me
            order = leaf >> 3
            for bit in range(bits):
                order = order + (((relative >> bit) & 1) << (bits - 1 - bit)) * parents
            return order

        def weights_of(index):
            base = pl.multiple_of(index * rows, 8)
            pairs = factor_ref[pl.ds(base, PLANE), :]
            pieces = [
                (factor_ref[pl.ds(base + PLANE + row, 1), :] * pairs).astype(jnp.bfloat16)
                for row in range(firsts)
            ]
            return jnp.concatenate(pieces, axis=0)

        for which in range(lists):

            def one(index, carry):
                product = jnp.dot(
                    weights_of(which * per_list + index),
                    block_refs[which][index],
                    preferred_element_type=jnp.float32,
                )
                sum_ref[slot_of(which, index)] += product
                return carry

            lax.fori_loop(0, per_list, one, 0, unroll=8)

        if last:

            def turned_back(slot):
                owner = slot // parents
                owner = owner // 2 + owner % 2 * (half // parents)
                return owner * parents + slot % parents

            def finish(slot, carry):
                for unit in range(units):
                    span = pl.ds(unit * SQUARE, SQUARE)
                    kept, sent = slot, half + slot
                    if unit < turned_units(units):
                        kept, sent = turned_back(kept), turned_back(sent)
                    keep_ref[unit, slot] = sum_ref[kept, span, :] + before_ref[kept, span, :]
                    send_ref[unit, slot] = (
                        sum_ref[sent, span, :] + before_ref[sent, span, :]
                    ).astype(jnp.bfloat16)
                return carry

            lax.fori_loop(0, half, finish, 0)

    whole = (slot_count, height, columns)
    scratch = [
        pltpu.VMEM((total * rows, block_size), jnp.float32),
        pltpu.VMEM((total * place_rows, block_size), jnp.float32),
        pltpu.VMEM((4, total, block_size), jnp.float32),
    ]
    out_shape = [jax.ShapeDtypeStruct(whole, jnp.float32)]
    if last:
        split = (units, half, SQUARE, columns)
        out_shape = [
            jax.ShapeDtypeStruct(split, jnp.float32),
            jax.ShapeDtypeStruct(split, jnp.bfloat16),
        ]
        scratch = [pltpu.VMEM(whole, jnp.float32)] + scratch
    operands = [waves, *numbers, *places, *blocks] + ([previous] if last else [])
    need = 3 * slot_count * height * columns * 4 + total * (rows + 12 + 64) * block_size * 4
    return pl.pallas_call(
        kernel,
        out_shape=out_shape,
        in_specs=[SMEM] * (1 + lists) + [VMEM] * (2 * lists + last),
        out_specs=[VMEM] * len(out_shape),
        scratch_shapes=scratch,
        compiler_params=pltpu.CompilerParams(vmem_limit_bytes=min(need + (3 << 20), 60 << 20)),
        cost_estimate=pl.CostEstimate(
            flops=2 * total * height * block_size * columns,
            bytes_accessed=total * block_size * columns * 2 + slot_count * height * columns * 4,
            transcendentals=0,
        ),
    )(*operands)


def rotate(sums, cone_waves):
    parents, units, square, columns = sums.shape
    cone_count = cone_waves.shape[1]
    digits = jnp.arange(square)
    digits = jnp.stack([digits // PLANE, digits // NODES % NODES, digits % NODES])
    nodes = jnp.cos((2.0 * digits.astype(jnp.float32) + 1.0) * (math.pi / (2.0 * NODES)))
    angle = 2.0 * (
        cone_waves[0][:, None] * nodes[0]
        + cone_waves[1][:, None] * nodes[1]
        + cone_waves[2][:, None] * nodes[2]
    )
    cosine, sine = jnp.cos(angle)[None, :, :, None], jnp.sin(angle)[None, :, :, None]
    parts = sums.reshape(parents, cone_count, 2, square, columns)
    real, imag = parts[:, :, 0], parts[:, :, 1]
    return jnp.stack([cosine * real - sine * imag, cosine * imag + sine * real], axis=2)


def mesh_flat():
    dirs = lax.axis_size("dir")
    return lax.axis_index("dom") * dirs + lax.axis_index("dir"), lax.axis_size("dom") * dirs


def greet_all():
    me, count = mesh_flat()
    dirs = lax.axis_size("dir")
    barrier = pltpu.get_barrier_semaphore()

    def one(offset, carry):
        peer = (me + offset) % count
        pl.semaphore_signal(
            barrier, inc=1, device_id=(peer // dirs, peer % dirs), device_id_type=MESH
        )
        return carry

    lax.fori_loop(1, count, one, 0)
    return barrier, count - 1


def send_rows(source, landing, width, send_sem, recv_sem):
    me, count = mesh_flat()
    dirs = lax.axis_size("dir")

    def one(offset, carry):
        peer = (me + offset) % count
        pltpu.make_async_remote_copy(
            src_ref=source.at[pl.ds(pl.multiple_of(peer * width, width), width)],
            dst_ref=landing.at[pl.ds(pl.multiple_of(me * width, width), width)],
            send_sem=send_sem,
            recv_sem=recv_sem,
            device_id=(peer // dirs, peer % dirs),
            device_id_type=MESH,
        ).start()
        return carry

    lax.fori_loop(1, count, one, 0)
    span = pl.ds(0, (count - 1) * width)
    peer = (me + 1) % count
    return pltpu.make_async_remote_copy(
        src_ref=source.at[span],
        dst_ref=landing.at[span],
        send_sem=send_sem,
        recv_sem=recv_sem,
        device_id=(peer // dirs, peer % dirs),
        device_id_type=MESH,
    )


def halo_rows(x_edges, send_list):
    owned_rows, columns = x_edges.shape
    partitions, width = send_list.shape

    def kernel(list_ref, x_ref, out_ref, table_ref, got_ref, send_ref, send_sem, recv_sem):
        barrier, others = greet_all()
        me, _ = mesh_flat()
        table_ref[...] = x_ref[...].astype(jnp.float32)

        def one(part, carry):
            start = pl.multiple_of(part * width, width)
            for lane in range(width):
                row = jnp.minimum(list_ref[part, lane], owned_rows - 1)
                got_ref[pl.ds(start + lane, 1), :] = table_ref[pl.ds(row, 1), :]
            return carry

        lax.fori_loop(0, partitions, one, 0)
        send_ref[...] = got_ref[...].astype(jnp.bfloat16)
        own = pl.ds(pl.multiple_of(me * width, width), width)
        out_ref[own, :] = jnp.zeros((width, columns), jnp.bfloat16)
        pl.semaphore_wait(barrier, others)
        whole = send_rows(send_ref, out_ref, width, send_sem, recv_sem)
        whole.wait_send()
        whole.wait_recv()

    return pl.pallas_call(
        kernel,
        out_shape=jax.ShapeDtypeStruct((partitions * width, columns), jnp.bfloat16),
        in_specs=[SMEM, VMEM],
        out_specs=VMEM,
        scratch_shapes=[
            pltpu.VMEM((owned_rows, columns), jnp.float32),
            pltpu.VMEM((partitions * width, columns), jnp.float32),
            pltpu.VMEM((partitions * width, columns), jnp.bfloat16),
            pltpu.SemaphoreType.DMA,
            pltpu.SemaphoreType.DMA,
        ],
        compiler_params=pltpu.CompilerParams(
            collective_id=0, has_side_effects=True, vmem_limit_bytes=16 << 20
        ),
        cost_estimate=pl.CostEstimate(
            flops=1_000_000_000, bytes_accessed=owned_rows * columns * 2, transcendentals=0
        ),
    )(send_list, x_edges)


def element_sums(links, live, x_edges, received, mats):
    element_count = mats.shape[1]
    edges = links.shape[0] // element_count
    owned_rows, columns = x_edges.shape
    halo = received.shape[0]
    table_rows = owned_rows + halo
    step = 8
    wide = 128

    def kernel(link_ref, live_ref, x_ref, halo_ref, mat_ref, own_ref, back_ref, *scratch):
        table_ref, term_ref = scratch[:2]
        got_refs, sums = scratch[2:4], scratch[4:]
        table_ref[pl.ds(0, owned_rows), :] = x_ref[...].astype(jnp.float32)
        table_ref[pl.ds(owned_rows, halo), :] = halo_ref[...].astype(jnp.float32)
        for ref in sums:
            ref[...] = jnp.zeros_like(ref)
        here = lax.broadcasted_iota(jnp.int32, (wide, wide), 0)
        there = lax.broadcasted_iota(jnp.int32, (wide, wide), 1)
        eye = jnp.where(here == there, 1.0, 0.0).astype(jnp.bfloat16)

        def fetch(number, got_ref):
            start = pl.multiple_of(number * wide, wide)
            for edge in range(edges):
                for lane in range(wide):
                    row = link_ref[start + (edge * element_count + lane)]
                    got_ref[pl.ds(edge * wide + lane, 1), :] = table_ref[pl.ds(row, 1), :]

        def product(number, got_ref):
            start = pl.multiple_of(number * wide, wide)
            count = start + lax.broadcasted_iota(jnp.int32, (1, wide), 1)
            live = count < live_ref[0]
            got = got_ref[...].astype(jnp.bfloat16)
            for i in range(edges):
                diagonals = []
                for j in range(edges):
                    row = mat_ref[pl.ds(edges * i + j, 1), pl.ds(start, wide)]
                    row = jnp.where(live, row, 0.0).astype(jnp.bfloat16)
                    diagonals.append(eye * row)
                term_ref[i, pl.ds(start, wide), :] = jnp.dot(
                    jnp.concatenate(diagonals, axis=1), got, preferred_element_type=jnp.float32
                )

        tiles = element_count // wide

        def products(index, carry):
            fetch(2 * index + 1, got_refs[1])
            product(2 * index, got_refs[0])
            fetch(jnp.minimum(2 * index + 2, tiles - 1), got_refs[0])
            product(2 * index + 1, got_refs[1])
            return carry

        fetch(0, got_refs[0])
        lax.fori_loop(0, tiles // 2, products, 0)

        def scatter(number, carry):
            start = pl.multiple_of(number * step, step)
            for lane in range(step):
                for edge in range(edges):
                    row = link_ref[start + (edge * element_count + lane)]
                    sums[edge][pl.ds(row, 1), :] += term_ref[edge, pl.ds(start + lane, 1), :]
            return carry

        lax.fori_loop(0, element_count // step, scatter, 0, unroll=2)

        def total_of(span):
            total = sums[0][span, :]
            for ref in sums[1:]:
                total = total + ref[span, :]
            return total

        own_ref[...] = total_of(pl.ds(0, owned_rows))
        back_ref[...] = total_of(pl.ds(owned_rows, halo)).astype(jnp.bfloat16)

    need = (edges + 4) * table_rows * columns * 4 + (6 << 20)
    return pl.pallas_call(
        kernel,
        out_shape=[
            jax.ShapeDtypeStruct((owned_rows, columns), jnp.float32),
            jax.ShapeDtypeStruct((halo, columns), jnp.bfloat16),
        ],
        in_specs=[SMEM, SMEM, VMEM, VMEM, VMEM],
        out_specs=[VMEM, VMEM],
        scratch_shapes=[
            pltpu.VMEM((table_rows, columns), jnp.float32),
            pltpu.VMEM((edges, element_count, columns), jnp.float32),
            pltpu.VMEM((edges * wide, columns), jnp.float32),
            pltpu.VMEM((edges * wide, columns), jnp.float32),
        ]
        + [pltpu.VMEM((table_rows, columns), jnp.float32)] * edges,
        compiler_params=pltpu.CompilerParams(vmem_limit_bytes=need),
        cost_estimate=pl.CostEstimate(
            flops=4_000_000_000, bytes_accessed=table_rows * columns * 8, transcendentals=0
        ),
    )(links, live, x_edges, received, mats)


def return_and_reduce(back, rows, keep, send, owned_rows, parents):
    partitions = lax.axis_size("dom") * lax.axis_size("dir")
    total_rows, columns = back.shape
    width = total_rows // partitions
    units, half, height, _ = keep.shape
    steps = log2(lax.axis_size("dom"))
    sizes = [half >> k for k in range(steps)]
    fold_step = 256
    lag = 3
    turned = turned_units(units)

    def kernel(row_ref, back_ref, keep_ref, send_ref, fold_ref, out_ref, *scratch):
        land_ref = scratch[0]
        got = scratch[1 : 1 + steps]
        keeps = [keep_ref] + list(scratch[1 + steps : 2 * steps])
        sends = [send_ref] + list(scratch[2 * steps : 3 * steps - 1])
        back_send, back_recv, send_sems, recv_sems = scratch[3 * steps - 1 :]
        me, _ = mesh_flat()
        dom = lax.axis_index("dom")
        barrier, others = greet_all()
        own = pl.ds(pl.multiple_of(me * width, width), width)
        land_ref[own, :] = jnp.zeros((width, columns), jnp.bfloat16)
        pl.semaphore_wait(barrier, others)
        def copy(k, unit):
            bit = 1 << ((k + 1) % steps if unit < turned else k)
            partner = dom + bit * (1 - 2 * ((dom // bit) % 2))
            return pltpu.make_async_remote_copy(
                src_ref=sends[k].at[unit],
                dst_ref=got[k].at[unit],
                send_sem=send_sems.at[k, unit],
                recv_sem=recv_sems.at[k, unit],
                device_id=(partner, lax.axis_index("dir")),
                device_id_type=MESH,
            )

        for unit in range(units):
            copy(0, unit).start()
        whole = send_rows(back_ref, land_ref, width, back_send, back_recv)

        def fold_all():
            whole.wait_recv()
            landed = land_ref[...]
            listed = row_ref[...]

            def fold(index, carry):
                start = pl.multiple_of(index * fold_step, fold_step)
                mine = start + lax.broadcasted_iota(jnp.int32, (fold_step, total_rows), 0)
                picks = jnp.where(mine == listed, 1.0, 0.0).astype(jnp.bfloat16)
                fold_ref[pl.ds(start, fold_step), :] = jnp.dot(
                    picks, landed, preferred_element_type=jnp.float32
                )
                return carry

            lax.fori_loop(0, owned_rows // fold_step, fold, 0)

        def step(k, unit):
            copy(k, unit).wait_recv()
            if k < steps - 1:
                low = sizes[k + 1]
                upper, lower = pl.ds(low, low), pl.ds(0, low)
                sends[k + 1][unit] = (
                    keeps[k][unit, upper] + got[k][unit, upper].astype(jnp.float32)
                ).astype(jnp.bfloat16)
                copy(k + 1, unit).start()
                keeps[k + 1][unit] = keeps[k][unit, lower] + got[k][unit, lower].astype(
                    jnp.float32
                )
            else:
                for parent in range(parents):
                    out_ref[parent, unit] = keeps[k][unit, parent] + got[k][unit, parent].astype(
                        jnp.float32
                    )

        for turn in range(units + lag * (steps - 1)):
            for k in reversed(range(steps)):
                unit = turn - lag * k
                if 0 <= unit < units and not (k == steps - 1 and unit < turned):
                    step(k, unit)
            if turn == units - 1 + lag * (steps - 2):
                for unit in range(turned):
                    step(steps - 1, unit)
                fold_all()
        whole.wait_send()
        for k in range(steps):
            for unit in range(units):
                copy(k, unit).wait_send()

    def buffers(dtype, first):
        return [pltpu.VMEM((units, size, height, columns), dtype) for size in sizes[first:]]

    scratch = (
        [pltpu.VMEM((total_rows, columns), jnp.bfloat16)]
        + buffers(jnp.bfloat16, 0)
        + buffers(jnp.float32, 1)
        + buffers(jnp.bfloat16, 1)
    )
    need = half * units * height * columns * 16 + total_rows * columns * 16 + (8 << 20)
    return pl.pallas_call(
        kernel,
        out_shape=[
            jax.ShapeDtypeStruct((owned_rows, columns), jnp.float32),
            jax.ShapeDtypeStruct((parents, units, height, columns), jnp.float32),
        ],
        in_specs=[VMEM] * 4,
        out_specs=[VMEM, VMEM],
        scratch_shapes=scratch
        + [
            pltpu.SemaphoreType.DMA,
            pltpu.SemaphoreType.DMA,
            pltpu.SemaphoreType.DMA((steps, units)),
            pltpu.SemaphoreType.DMA((steps, units)),
        ],
        compiler_params=pltpu.CompilerParams(
            collective_id=1, has_side_effects=True, vmem_limit_bytes=min(need, 60 << 20)
        ),
        cost_estimate=pl.CostEstimate(
            flops=2 * owned_rows * total_rows * columns,
            bytes_accessed=half * units * height * columns * 6,
            transcendentals=0,
        ),
    )(rows, back, keep, send)


def shards(
    x_edges,
    send_list,
    connectivity,
    elem_mats,
    elem_live,
    currents,
    positions,
    block_live,
    block_owner,
    block_leaf,
    cone_waves,
):
    dom_count, dir_count = lax.axis_size("dom"), lax.axis_size("dir")
    parents = LEAVES_DEV // OCTANTS
    slot_count = dom_count * parents
    dir_bits = log2(dir_count)
    cone_count = cone_waves.shape[1]
    owned_rows = x_edges.shape[0]

    numbers = jnp.stack([block_leaf, block_live, block_owner])
    own = (numbers, positions, currents)
    near_bits = list(range(dir_bits - 1))
    near = [spread(value, "dir", near_bits) for value in own]
    received = halo_rows(x_edges, send_list)
    late, received = lax.optimization_barrier((currents, received))
    own = (numbers, positions, late)
    far = [lax.ppermute(value, "dir", xor_pairs(dir_count, dir_bits - 1)) for value in own]
    owned, back = element_sums(connectivity.reshape(-1), elem_live, x_edges, received, elem_mats)
    (sums,) = block_sums(cone_waves, *near, None, slot_count, cone_count)
    *far, back = lax.optimization_barrier((*far, back))
    far = [spread(value, "dir", near_bits) for value in far]
    keep, send = block_sums(cone_waves, *far, sums, slot_count, cone_count)
    fold, sums = return_and_reduce(
        back, send_list.reshape(1, -1), keep, send, owned_rows, parents
    )
    return owned + fold, rotate(sums, cone_waves)


def solution(mesh):
    placed = (
        P(("dom", "dir"), None),
        P(("dom", "dir"), None),
        P(None, ("dom", "dir")),
        P(None, ("dom", "dir")),
        P(("dom", "dir")),
        P(("dom", "dir"), None, None),
        P(("dom", "dir"), None, None),
        P(("dom", "dir")),
        P(("dom", "dir")),
        P(("dom", "dir")),
        P(None, "dir"),
    )
    return jax.shard_map(
        shards,
        mesh=mesh,
        in_specs=placed,
        out_specs=(P(("dom", "dir"), None), P("dom", "dir", None, None, None)),
        check_vma=False,
    )
```

```python
import math

import jax
import jax.numpy as jnp
from jax import lax
from jax.experimental import pallas as pl
from jax.experimental.pallas import tpu as pltpu
from jax.sharding import PartitionSpec as P

LEAVES_DEV = 16
OCTANTS = 8
NODES = 4
PLANE = NODES * NODES
SQUARE = NODES**3
POINTS = [math.cos((2 * j + 1) * math.pi / (2 * NODES)) for j in range(NODES)]
MESH = pl.DeviceIdType.MESH
VMEM = pl.BlockSpec(memory_space=pltpu.VMEM)
SMEM = pl.BlockSpec(memory_space=pltpu.SMEM)


def lagrange_rows(v):
    rows = []
    for target in range(NODES):
        product = None
        scale = 1.0
        for other in range(NODES):
            if other != target:
                factor = v - POINTS[other]
                product = factor if product is None else product * factor
                scale *= POINTS[target] - POINTS[other]
        rows.append(product * (1.0 / scale))
    return rows


def cos_sin(phase):
    turns = jnp.floor(phase * (1.0 / math.pi) + 0.5)
    odd = turns - 2.0 * jnp.floor(turns * 0.5)
    sign = 1.0 - 2.0 * odd
    high = 3.140625
    rest = (phase - turns * high) - turns * (math.pi - high)
    square = rest * rest
    cosine = jnp.full_like(rest, 1.0 / math.factorial(12))
    for order in (10, 8, 6, 4, 2, 0):
        cosine = cosine * square + (1.0 if order % 4 == 0 else -1.0) / math.factorial(order)
    sine = jnp.full_like(rest, -1.0 / math.factorial(11))
    for order in (9, 7, 5, 3, 1):
        sine = sine * square + (1.0 if order % 4 == 1 else -1.0) / math.factorial(order)
    return cosine * sign, sine * rest * sign


def xor_pairs(count, bit):
    return [(i, i ^ (1 << bit)) for i in range(count)]


def log2(count):
    bits = count.bit_length() - 1
    if count != 1 << bits:
        raise ValueError("axis size")
    return bits


def turned_units(units):
    return units // 4


def spread(value, axis, bits):
    held = [value]
    count = lax.axis_size(axis)
    for bit in bits:
        held = held + [lax.ppermute(h, axis, xor_pairs(count, bit)) for h in held]
    return held


def block_sums(waves, numbers, places, blocks, previous, slot_count, cone_count):
    last = previous is not None
    units = 2 * cone_count
    lists = len(blocks)
    per_list, block_size, columns = blocks[0].shape
    total = lists * per_list
    height = units * SQUARE
    firsts = units * NODES
    rows = PLANE + firsts + 8
    group = 16
    place_rows = 8
    half = slot_count // 2
    parents = LEAVES_DEV // OCTANTS

    def kernel(*refs):
        wave_ref = refs[0]
        number_refs = refs[1 : 1 + lists]
        place_refs = refs[1 + lists : 1 + 2 * lists]
        block_refs = refs[1 + 2 * lists : 1 + 3 * lists]
        at = 1 + 3 * lists
        if last:
            before_ref, keep_ref, send_ref, sum_ref = refs[at : at + 4]
        else:
            sum_ref = refs[at]
        factor_ref, place_ref, number_ref = refs[-3:]

        for which in range(lists):

            def unpack(index, carry):
                at_block = which * per_list + index
                place = place_refs[which][index].astype(jnp.float32)
                place_ref[pl.ds(pl.multiple_of(at_block * place_rows, place_rows), 3), :] = place
                leaf = number_refs[which][0, index]
                shifts = [(leaf >> 2) & 1, (leaf >> 1) & 1, leaf & 1]
                values = [(2 * shift - 1).astype(jnp.float32) for shift in shifts]
                values.append(number_refs[which][1, index].astype(jnp.float32))
                for row, value in enumerate(values):
                    number_ref[row, pl.ds(at_block, 1), :] = jnp.full(
                        (1, block_size), value, jnp.float32
                    )
                return carry

            lax.fori_loop(0, per_list, unpack, 0, unroll=4)

        lanes = lax.broadcasted_iota(jnp.int32, (group, block_size), 1).astype(jnp.float32)
        for part in range(total // group):
            span = pl.ds(part * group, group)
            double = [
                number_ref[d, span, :]
                + place_ref[pl.ds(part * group * place_rows + d, group, stride=place_rows), :]
                for d in range(3)
            ]
            live = lanes < number_ref[3, span, :]
            first = [jnp.where(live, r, 0.0) for r in lagrange_rows(0.5 * double[0])]
            second = lagrange_rows(0.5 * double[1])
            third = lagrange_rows(0.5 * double[2])
            start = part * group * rows

            def put(row, value):
                factor_ref[pl.ds(start + row, group, stride=rows), :] = value

            for a in range(NODES):
                for b in range(NODES):
                    put(a * NODES + b, second[a] * third[b])
            for cone in range(cone_count):
                phase = (
                    wave_ref[0, cone] * double[0]
                    + wave_ref[1, cone] * double[1]
                    + wave_ref[2, cone] * double[2]
                )
                cosine, sine = cos_sin(phase)
                for digit in range(NODES):
                    put(PLANE + cone * 2 * NODES + digit, first[digit] * cosine)
                    put(PLANE + cone * 2 * NODES + NODES + digit, first[digit] * -sine)

        sum_ref[...] = jnp.zeros_like(sum_ref)
        me = lax.axis_index("dom")
        bits = log2(lax.axis_size("dom"))

        def slot_of(which, index):
            leaf, owner = number_refs[which][0, index], number_refs[which][2, index]
            relative = owner ^ me
            order = leaf >> 3
            for bit in range(bits):
                order = order + (((relative >> bit) & 1) << (bits - 1 - bit)) * parents
            return order

        def weights_of(index):
            base = pl.multiple_of(index * rows, 8)
            pairs = factor_ref[pl.ds(base, PLANE), :]
            pieces = [
                (factor_ref[pl.ds(base + PLANE + row, 1), :] * pairs).astype(jnp.bfloat16)
                for row in range(firsts)
            ]
            return jnp.concatenate(pieces, axis=0)

        for which in range(lists):

            def one(index, carry):
                product = jnp.dot(
                    weights_of(which * per_list + index),
                    block_refs[which][index],
                    preferred_element_type=jnp.float32,
                )
                sum_ref[slot_of(which, index)] += product
                return carry

            lax.fori_loop(0, per_list, one, 0, unroll=8)

        if last:

            def turned_back(slot):
                owner = slot // parents
                owner = owner // 2 + owner % 2 * (half // parents)
                return owner * parents + slot % parents

            def finish(slot, carry):
                for unit in range(units):
                    span = pl.ds(unit * SQUARE, SQUARE)
                    kept, sent = slot, half + slot
                    if unit < turned_units(units):
                        kept, sent = turned_back(kept), turned_back(sent)
                    keep_ref[unit, slot] = sum_ref[kept, span, :] + before_ref[kept, span, :]
                    send_ref[unit, slot] = (
                        sum_ref[sent, span, :] + before_ref[sent, span, :]
                    ).astype(jnp.bfloat16)
                return carry

            lax.fori_loop(0, half, finish, 0)

    whole = (slot_count, height, columns)
    scratch = [
        pltpu.VMEM((total * rows, block_size), jnp.float32),
        pltpu.VMEM((total * place_rows, block_size), jnp.float32),
        pltpu.VMEM((4, total, block_size), jnp.float32),
    ]
    out_shape = [jax.ShapeDtypeStruct(whole, jnp.float32)]
    if last:
        split = (units, half, SQUARE, columns)
        out_shape = [
            jax.ShapeDtypeStruct(split, jnp.float32),
            jax.ShapeDtypeStruct(split, jnp.bfloat16),
        ]
        scratch = [pltpu.VMEM(whole, jnp.float32)] + scratch
    operands = [waves, *numbers, *places, *blocks] + ([previous] if last else [])
    need = 3 * slot_count * height * columns * 4 + total * (rows + 12 + 64) * block_size * 4
    return pl.pallas_call(
        kernel,
        out_shape=out_shape,
        in_specs=[SMEM] * (1 + lists) + [VMEM] * (2 * lists + last),
        out_specs=[VMEM] * len(out_shape),
        scratch_shapes=scratch,
        compiler_params=pltpu.CompilerParams(vmem_limit_bytes=min(need + (3 << 20), 60 << 20)),
        cost_estimate=pl.CostEstimate(
            flops=2 * total * height * block_size * columns,
            bytes_accessed=total * block_size * columns * 2 + slot_count * height * columns * 4,
            transcendentals=0,
        ),
    )(*operands)


def rotate(sums, cone_waves):
    parents, units, square, columns = sums.shape
    cone_count = cone_waves.shape[1]
    digits = jnp.arange(square)
    digits = jnp.stack([digits // PLANE, digits // NODES % NODES, digits % NODES])
    nodes = jnp.cos((2.0 * digits.astype(jnp.float32) + 1.0) * (math.pi / (2.0 * NODES)))
    angle = 2.0 * (
        cone_waves[0][:, None] * nodes[0]
        + cone_waves[1][:, None] * nodes[1]
        + cone_waves[2][:, None] * nodes[2]
    )
    cosine, sine = jnp.cos(angle)[None, :, :, None], jnp.sin(angle)[None, :, :, None]
    parts = sums.reshape(parents, cone_count, 2, square, columns)
    real, imag = parts[:, :, 0], parts[:, :, 1]
    return jnp.stack([cosine * real - sine * imag, cosine * imag + sine * real], axis=2)


def mesh_flat():
    dirs = lax.axis_size("dir")
    return lax.axis_index("dom") * dirs + lax.axis_index("dir"), lax.axis_size("dom") * dirs


def greet_all():
    me, count = mesh_flat()
    dirs = lax.axis_size("dir")
    barrier = pltpu.get_barrier_semaphore()

    def one(offset, carry):
        peer = (me + offset) % count
        pl.semaphore_signal(
            barrier, inc=1, device_id=(peer // dirs, peer % dirs), device_id_type=MESH
        )
        return carry

    lax.fori_loop(1, count, one, 0)
    return barrier, count - 1


def send_rows(source, landing, width, send_sem, recv_sem):
    me, count = mesh_flat()
    dirs = lax.axis_size("dir")

    def one(offset, carry):
        peer = (me + offset) % count
        pltpu.make_async_remote_copy(
            src_ref=source.at[pl.ds(pl.multiple_of(peer * width, width), width)],
            dst_ref=landing.at[pl.ds(pl.multiple_of(me * width, width), width)],
            send_sem=send_sem,
            recv_sem=recv_sem,
            device_id=(peer // dirs, peer % dirs),
            device_id_type=MESH,
        ).start()
        return carry

    lax.fori_loop(1, count, one, 0)
    span = pl.ds(0, (count - 1) * width)
    peer = (me + 1) % count
    return pltpu.make_async_remote_copy(
        src_ref=source.at[span],
        dst_ref=landing.at[span],
        send_sem=send_sem,
        recv_sem=recv_sem,
        device_id=(peer // dirs, peer % dirs),
        device_id_type=MESH,
    )


def halo_rows(x_edges, send_list):
    owned_rows, columns = x_edges.shape
    partitions, width = send_list.shape

    def kernel(list_ref, x_ref, out_ref, table_ref, got_ref, send_ref, send_sem, recv_sem):
        barrier, others = greet_all()
        me, _ = mesh_flat()
        table_ref[...] = x_ref[...].astype(jnp.float32)

        def one(part, carry):
            start = pl.multiple_of(part * width, width)
            for lane in range(width):
                row = jnp.minimum(list_ref[part, lane], owned_rows - 1)
                got_ref[pl.ds(start + lane, 1), :] = table_ref[pl.ds(row, 1), :]
            return carry

        lax.fori_loop(0, partitions, one, 0)
        send_ref[...] = got_ref[...].astype(jnp.bfloat16)
        own = pl.ds(pl.multiple_of(me * width, width), width)
        out_ref[own, :] = jnp.zeros((width, columns), jnp.bfloat16)
        pl.semaphore_wait(barrier, others)
        whole = send_rows(send_ref, out_ref, width, send_sem, recv_sem)
        whole.wait_send()
        whole.wait_recv()

    return pl.pallas_call(
        kernel,
        out_shape=jax.ShapeDtypeStruct((partitions * width, columns), jnp.bfloat16),
        in_specs=[SMEM, VMEM],
        out_specs=VMEM,
        scratch_shapes=[
            pltpu.VMEM((owned_rows, columns), jnp.float32),
            pltpu.VMEM((partitions * width, columns), jnp.float32),
            pltpu.VMEM((partitions * width, columns), jnp.bfloat16),
            pltpu.SemaphoreType.DMA,
            pltpu.SemaphoreType.DMA,
        ],
        compiler_params=pltpu.CompilerParams(
            collective_id=0, has_side_effects=True, vmem_limit_bytes=16 << 20
        ),
        cost_estimate=pl.CostEstimate(
            flops=1_000_000_000, bytes_accessed=owned_rows * columns * 2, transcendentals=0
        ),
    )(send_list, x_edges)


def element_sums(links, live, x_edges, received, mats):
    element_count = mats.shape[1]
    edges = links.shape[0] // element_count
    owned_rows, columns = x_edges.shape
    halo = received.shape[0]
    table_rows = owned_rows + halo
    step = 8
    wide = 128

    def kernel(link_ref, live_ref, x_ref, halo_ref, mat_ref, own_ref, back_ref, *scratch):
        table_ref, term_ref = scratch[:2]
        got_refs, sums = scratch[2:4], scratch[4:]
        table_ref[pl.ds(0, owned_rows), :] = x_ref[...].astype(jnp.float32)
        table_ref[pl.ds(owned_rows, halo), :] = halo_ref[...].astype(jnp.float32)
        for ref in sums:
            ref[...] = jnp.zeros_like(ref)
        here = lax.broadcasted_iota(jnp.int32, (wide, wide), 0)
        there = lax.broadcasted_iota(jnp.int32, (wide, wide), 1)
        eye = jnp.where(here == there, 1.0, 0.0).astype(jnp.bfloat16)

        def fetch(number, got_ref):
            start = pl.multiple_of(number * wide, wide)
            for edge in range(edges):
                for lane in range(wide):
                    row = link_ref[start + (edge * element_count + lane)]
                    got_ref[pl.ds(edge * wide + lane, 1), :] = table_ref[pl.ds(row, 1), :]

        def product(number, got_ref):
            start = pl.multiple_of(number * wide, wide)
            count = start + lax.broadcasted_iota(jnp.int32, (1, wide), 1)
            live = count < live_ref[0]
            got = got_ref[...].astype(jnp.bfloat16)
            for i in range(edges):
                diagonals = []
                for j in range(edges):
                    row = mat_ref[pl.ds(edges * i + j, 1), pl.ds(start, wide)]
                    row = jnp.where(live, row, 0.0).astype(jnp.bfloat16)
                    diagonals.append(eye * row)
                term_ref[i, pl.ds(start, wide), :] = jnp.dot(
                    jnp.concatenate(diagonals, axis=1), got, preferred_element_type=jnp.float32
                )

        tiles = element_count // wide

        def products(index, carry):
            fetch(2 * index + 1, got_refs[1])
            product(2 * index, got_refs[0])
            fetch(jnp.minimum(2 * index + 2, tiles - 1), got_refs[0])
            product(2 * index + 1, got_refs[1])
            return carry

        fetch(0, got_refs[0])
        lax.fori_loop(0, tiles // 2, products, 0)

        def scatter(number, carry):
            start = pl.multiple_of(number * step, step)
            for lane in range(step):
                for edge in range(edges):
                    row = link_ref[start + (edge * element_count + lane)]
                    sums[edge][pl.ds(row, 1), :] += term_ref[edge, pl.ds(start + lane, 1), :]
            return carry

        lax.fori_loop(0, element_count // step, scatter, 0, unroll=2)

        def total_of(span):
            total = sums[0][span, :]
            for ref in sums[1:]:
                total = total + ref[span, :]
            return total

        own_ref[...] = total_of(pl.ds(0, owned_rows))
        back_ref[...] = total_of(pl.ds(owned_rows, halo)).astype(jnp.bfloat16)

    need = (edges + 4) * table_rows * columns * 4 + (6 << 20)
    return pl.pallas_call(
        kernel,
        out_shape=[
            jax.ShapeDtypeStruct((owned_rows, columns), jnp.float32),
            jax.ShapeDtypeStruct((halo, columns), jnp.bfloat16),
        ],
        in_specs=[SMEM, SMEM, VMEM, VMEM, VMEM],
        out_specs=[VMEM, VMEM],
        scratch_shapes=[
            pltpu.VMEM((table_rows, columns), jnp.float32),
            pltpu.VMEM((edges, element_count, columns), jnp.float32),
            pltpu.VMEM((edges * wide, columns), jnp.float32),
            pltpu.VMEM((edges * wide, columns), jnp.float32),
        ]
        + [pltpu.VMEM((table_rows, columns), jnp.float32)] * edges,
        compiler_params=pltpu.CompilerParams(vmem_limit_bytes=need),
        cost_estimate=pl.CostEstimate(
            flops=4_000_000_000, bytes_accessed=table_rows * columns * 8, transcendentals=0
        ),
    )(links, live, x_edges, received, mats)


def return_and_reduce(back, rows, keep, send, owned_rows, parents):
    partitions = lax.axis_size("dom") * lax.axis_size("dir")
    total_rows, columns = back.shape
    width = total_rows // partitions
    units, half, height, _ = keep.shape
    steps = log2(lax.axis_size("dom"))
    sizes = [half >> k for k in range(steps)]
    fold_step = 256
    lag = 4
    turned = turned_units(units)

    def kernel(row_ref, back_ref, keep_ref, send_ref, fold_ref, out_ref, *scratch):
        land_ref = scratch[0]
        got = scratch[1 : 1 + steps]
        keeps = [keep_ref] + list(scratch[1 + steps : 2 * steps])
        sends = [send_ref] + list(scratch[2 * steps : 3 * steps - 1])
        back_send, back_recv, send_sems, recv_sems = scratch[3 * steps - 1 :]
        me, _ = mesh_flat()
        dom = lax.axis_index("dom")
        barrier, others = greet_all()
        own = pl.ds(pl.multiple_of(me * width, width), width)
        land_ref[own, :] = jnp.zeros((width, columns), jnp.bfloat16)
        pl.semaphore_wait(barrier, others)
        def copy(k, unit):
            bit = 1 << ((k + 1) % steps if unit < turned else k)
            partner = dom + bit * (1 - 2 * ((dom // bit) % 2))
            return pltpu.make_async_remote_copy(
                src_ref=sends[k].at[unit],
                dst_ref=got[k].at[unit],
                send_sem=send_sems.at[k, unit],
                recv_sem=recv_sems.at[k, unit],
                device_id=(partner, lax.axis_index("dir")),
                device_id_type=MESH,
            )

        for unit in range(units):
            copy(0, unit).start()
        whole = send_rows(back_ref, land_ref, width, back_send, back_recv)

        def fold_all():
            whole.wait_recv()
            landed = land_ref[...]
            listed = row_ref[...]

            def fold(index, carry):
                start = pl.multiple_of(index * fold_step, fold_step)
                mine = start + lax.broadcasted_iota(jnp.int32, (fold_step, total_rows), 0)
                picks = jnp.where(mine == listed, 1.0, 0.0).astype(jnp.bfloat16)
                fold_ref[pl.ds(start, fold_step), :] = jnp.dot(
                    picks, landed, preferred_element_type=jnp.float32
                )
                return carry

            lax.fori_loop(0, owned_rows // fold_step, fold, 0)

        def step(k, unit):
            copy(k, unit).wait_recv()
            if k < steps - 1:
                low = sizes[k + 1]
                upper, lower = pl.ds(low, low), pl.ds(0, low)
                sends[k + 1][unit] = (
                    keeps[k][unit, upper] + got[k][unit, upper].astype(jnp.float32)
                ).astype(jnp.bfloat16)
                copy(k + 1, unit).start()
                keeps[k + 1][unit] = keeps[k][unit, lower] + got[k][unit, lower].astype(
                    jnp.float32
                )
            else:
                for parent in range(parents):
                    out_ref[parent, unit] = keeps[k][unit, parent] + got[k][unit, parent].astype(
                        jnp.float32
                    )

        for turn in range(units + lag * (steps - 1)):
            for k in reversed(range(steps)):
                unit = turn - lag * k
                if 0 <= unit < units and not (k == steps - 1 and unit < turned):
                    step(k, unit)
            if turn == units - 1 + lag * (steps - 2):
                for unit in range(turned):
                    step(steps - 1, unit)
                fold_all()
        whole.wait_send()
        for k in range(steps):
            for unit in range(units):
                copy(k, unit).wait_send()

    def buffers(dtype, first):
        return [pltpu.VMEM((units, size, height, columns), dtype) for size in sizes[first:]]

    scratch = (
        [pltpu.VMEM((total_rows, columns), jnp.bfloat16)]
        + buffers(jnp.bfloat16, 0)
        + buffers(jnp.float32, 1)
        + buffers(jnp.bfloat16, 1)
    )
    need = half * units * height * columns * 16 + total_rows * columns * 16 + (8 << 20)
    return pl.pallas_call(
        kernel,
        out_shape=[
            jax.ShapeDtypeStruct((owned_rows, columns), jnp.float32),
            jax.ShapeDtypeStruct((parents, units, height, columns), jnp.float32),
        ],
        in_specs=[VMEM] * 4,
        out_specs=[VMEM, VMEM],
        scratch_shapes=scratch
        + [
            pltpu.SemaphoreType.DMA,
            pltpu.SemaphoreType.DMA,
            pltpu.SemaphoreType.DMA((steps, units)),
            pltpu.SemaphoreType.DMA((steps, units)),
        ],
        compiler_params=pltpu.CompilerParams(
            collective_id=1, has_side_effects=True, vmem_limit_bytes=min(need, 60 << 20)
        ),
        cost_estimate=pl.CostEstimate(
            flops=2 * owned_rows * total_rows * columns,
            bytes_accessed=half * units * height * columns * 6,
            transcendentals=0,
        ),
    )(rows, back, keep, send)


def shards(
    x_edges,
    send_list,
    connectivity,
    elem_mats,
    elem_live,
    currents,
    positions,
    block_live,
    block_owner,
    block_leaf,
    cone_waves,
):
    dom_count, dir_count = lax.axis_size("dom"), lax.axis_size("dir")
    parents = LEAVES_DEV // OCTANTS
    slot_count = dom_count * parents
    dir_bits = log2(dir_count)
    cone_count = cone_waves.shape[1]
    owned_rows = x_edges.shape[0]

    numbers = jnp.stack([block_leaf, block_live, block_owner])
    own = (numbers, positions, currents)
    near_bits = list(range(dir_bits - 1))
    near = [spread(value, "dir", near_bits) for value in own]
    received = halo_rows(x_edges, send_list)
    late, received = lax.optimization_barrier((currents, received))
    own = (numbers, positions, late)
    far = [lax.ppermute(value, "dir", xor_pairs(dir_count, dir_bits - 1)) for value in own]
    owned, back = element_sums(connectivity.reshape(-1), elem_live, x_edges, received, elem_mats)
    (sums,) = block_sums(cone_waves, *near, None, slot_count, cone_count)
    *far, back = lax.optimization_barrier((*far, back))
    far = [spread(value, "dir", near_bits) for value in far]
    keep, send = block_sums(cone_waves, *far, sums, slot_count, cone_count)
    fold, sums = return_and_reduce(
        back, send_list.reshape(1, -1), keep, send, owned_rows, parents
    )
    return owned + fold, rotate(sums, cone_waves)


def solution(mesh):
    placed = (
        P(("dom", "dir"), None),
        P(("dom", "dir"), None),
        P(None, ("dom", "dir")),
        P(None, ("dom", "dir")),
        P(("dom", "dir")),
        P(("dom", "dir"), None, None),
        P(("dom", "dir"), None, None),
        P(("dom", "dir")),
        P(("dom", "dir")),
        P(("dom", "dir")),
        P(None, "dir"),
    )
    return jax.shard_map(
        shards,
        mesh=mesh,
        in_specs=placed,
        out_specs=(P(("dom", "dir"), None), P("dom", "dir", None, None, None)),
        check_vma=False,
    )
```
